32 devices in a mesh: groups: 1, blk: 16 (over z, y, x), head: 2 (over core).
Axes of the slice: x: 2, y: 2, z: 4, core: 2. Of those that a mesh axis runs over, the one named last changes fastest.
Arguments:
- queries: bfloat16 [128, 8192], P(('groups', 'blk'), 'head'), may hold values from -6 to 6
- key_cache: bfloat16 [2, 32768, 8, 128], P('groups', 'blk', 'head'), may hold values from -18 to 18
- value_cache: bfloat16 [2, 32768, 8, 128], P('groups', 'blk', 'head'), may hold values from -6 to 6
- lengths: int32 [2], P('groups'), may hold values from 0 to 32704
- residual: bfloat16 [128, 8192], P('groups', 'blk'), may hold values from -6 to 6
- out_weight: bfloat16 [8192, 8192], P('head', 'blk'), may hold values from -0.0625 to 0.0625
- norm_gain: bfloat16 [8192], P('blk'), may hold values from 0.099609375 to 1.8984375
- gate_weight: bfloat16 [8192, 16384], P(None, ('head', 'blk')), may hold values from -0.0625 to 0.0625
- up_weight: bfloat16 [8192, 16384], P(None, ('head', 'blk')), may hold values from -0.0625 to 0.0625
- down_weight: bfloat16 [16384, 8192], P('head', 'blk'), may hold values from -0.046875 to 0.046875
Outputs:
- layer_out: bfloat16 [128, 8192], P('groups', 'blk')
The draws below stay inside these ranges and needn't reach their ends.
Inputs may be any that keep to these rules, and one draw needn't show every extreme that they name: lengths[b] + 64 <= 32768; the cache holds sequence b's new keys and values at positions lengths[b] to lengths[b] + 63.
All inputs are finite; a program needn't handle non-finite values.
Results may differ from the reference program's by a relative error of at most 0.01.
Values may be sent and summed in bfloat16 or wider, within the bound.
No kernel may reach another device: no remote copies, remote signals or barrier semaphores. Data moves between devices by JAX's collectives and lax.ppermute only.
A program may use at most 128 MiB of HBM per device.

```python
import jax
import jax.numpy as jnp
from jax import lax

D = 8192
HQ = 64
KVH = 8
HD = 128
FF = 16384
B = 2
Q = 64
CTX_DEV = 2048
CTX = 32768
ROWS = 128
N_BLK = 16


def draw_queries(key, part):
    values = jnp.clip(jax.random.normal(key, (ROWS, HQ * HD), jnp.float32), -6.0, 6.0)
    return values.astype(jnp.bfloat16)


def draw_key_cache(key, part):
    values = jnp.clip(3.0 * jax.random.normal(key, (B, CTX, KVH, HD), jnp.float32), -18.0, 18.0)
    return values.astype(jnp.bfloat16)


def levels(own_key, shape, split, low, largest):
    def one(dim, parts):
        draws = jax.random.uniform(jax.random.fold_in(jax.random.fold_in(own_key, 6), dim), (parts,), jnp.float32, low / len(split), largest / len(split))
        return jnp.repeat(jnp.exp(draws), shape[dim] // parts).reshape((-1,) + (1,) * (len(shape) - dim - 1))

    gain = one(*split[0])
    for cut in split[1:]:
        gain = gain * one(*cut)
    return gain


def noise(rng, extent, deviation, bound, shards=(), kind=jnp.bfloat16):
    result = deviation * jax.random.normal(rng, extent, jnp.float32)
    if shards:
        result = result * levels(rng, extent, shards, -0.22, 0.18)
    return jnp.clip(result, -bound, bound).astype(kind)


def setup_inputs(seed: int = 0, part: int = 0) -> dict:
    splits = jax.random.split(jax.random.key(seed), 11)
    part_splits = jax.random.split(jax.random.fold_in(splits[10], part), 11)
    queries = draw_queries(jax.random.fold_in(jax.random.fold_in(splits[10], part), 71), part)
    key_cache = draw_key_cache(jax.random.fold_in(jax.random.fold_in(splits[10], part), 71), part)
    value_cache = noise(part_splits[2], (B, CTX, KVH, HD), 1.0, 6.0, ((1, 16), (2, 2)))
    lengths = jax.random.randint(part_splits[3], (B,), 0, CTX - Q + 1).astype(jnp.int32)
    residual = noise(part_splits[4], (ROWS, D), 1.0, 6.0, ((1, 16),))
    out_weight = noise(splits[5], (HQ * HD, D), (HQ * HD) ** -0.5, 0.0625, ((0, 2), (1, 16)))
    norm_gain = jnp.clip(1.0 + 0.18 * jax.random.normal(splits[6], (D,), jnp.float32), 0.099609375, 1.8984375).astype(jnp.bfloat16)
    gate_weight = noise(splits[7], (D, FF), D ** -0.5, 0.0625, ((1, 32),))
    up_weight = noise(splits[8], (D, FF), D ** -0.5, 0.0625, ((1, 32),))
    down_weight = noise(splits[9], (FF, D), FF ** -0.5, 0.046875, ((0, 2), (1, 16)))
    return {"queries": queries, "key_cache": key_cache, "value_cache": value_cache, "lengths": lengths, "residual": residual, "out_weight": out_weight, "norm_gain": norm_gain, "gate_weight": gate_weight, "up_weight": up_weight, "down_weight": down_weight}


neg_big = -1e+30
epsilon = 1e-06

def merge_stats(first, second):
    first_max, first_sum, first_out = first
    second_max, second_sum, second_out = second
    top = jnp.maximum(first_max, second_max)
    first_scale = jnp.exp(first_max - top)
    second_scale = jnp.exp(second_max - top)
    total_sum = first_sum * first_scale + second_sum * second_scale
    total_out = first_out * first_scale[..., None] + second_out * second_scale[..., None]
    return (top, total_sum, total_out)

def reference(queries, key_cache, value_cache, lengths, residual, out_weight, norm_gain, gate_weight, up_weight, down_weight):
    group_size = HQ // KVH
    shaped = queries.astype(jnp.float32).reshape(B, Q, KVH, group_size, HD)
    query_pos = lengths[:, None].astype(jnp.int32) + jnp.arange(Q, dtype=jnp.int32)[None, :]
    scale = HD ** (-0.5)

    def one_block(carry, block_index):
        first = (block_index * CTX_DEV).astype(jnp.int32)
        keys = lax.dynamic_slice_in_dim(key_cache, first, CTX_DEV, 1).astype(jnp.float32)
        values = lax.dynamic_slice_in_dim(value_cache, first, CTX_DEV, 1).astype(jnp.float32)
        key_pos = first + jnp.arange(CTX_DEV, dtype=jnp.int32)
        scores = jnp.einsum('bqkgd,bckd->bqkgc', shaped, keys) * scale
        visible = key_pos[None, None, None, None, :] <= query_pos[:, :, None, None, None]
        block_max = lax.optimization_barrier(jnp.max(jnp.where(visible, scores, neg_big), axis=-1))
        weights = jnp.where(visible, jnp.exp(scores - block_max[..., None]), 0.0)
        block_sum = lax.optimization_barrier(jnp.sum(weights, axis=-1))
        rounded = lax.optimization_barrier(weights.astype(jnp.bfloat16)).astype(jnp.float32)
        block_out = jnp.einsum('bqkgc,bckd->bqkgd', rounded, values)
        block_mean = block_out / jnp.maximum(block_sum, 1.0)[..., None]
        block_mean = lax.optimization_barrier(block_mean.astype(jnp.bfloat16)).astype(jnp.float32)
        contribution = block_mean * block_sum[..., None]
        return (merge_stats(carry, (block_max, block_sum, contribution)), None)
    start = (jnp.full((B, Q, KVH, group_size), neg_big, jnp.float32), jnp.zeros((B, Q, KVH, group_size), jnp.float32), jnp.zeros((B, Q, KVH, group_size, HD), jnp.float32))
    final, unused = lax.scan(one_block, start, jnp.arange(N_BLK, dtype=jnp.int32))
    attn = (final[2] / final[1][..., None]).astype(jnp.bfloat16).reshape(ROWS, HQ * HD)
    stream = residual.astype(jnp.float32) + jnp.dot(attn, out_weight, preferred_element_type=jnp.float32)
    squares = lax.optimization_barrier(jnp.sum(stream * stream, axis=1))
    normed = (stream * lax.rsqrt(squares / D + epsilon)[:, None] * norm_gain.astype(jnp.float32)[None, :]).astype(jnp.bfloat16)
    gate = jnp.dot(normed, gate_weight, preferred_element_type=jnp.float32)
    up = jnp.dot(normed, up_weight, preferred_element_type=jnp.float32)
    hidden = (jax.nn.silu(gate) * up).astype(jnp.bfloat16)
    down = jnp.dot(hidden, down_weight, preferred_element_type=jnp.float32)
    return (stream + down).astype(jnp.bfloat16)
```

```python
import functools

import jax
import jax.numpy as jnp
from jax import lax
from jax.experimental import pallas as pl
from jax.experimental.pallas import tpu as pltpu
from jax.sharding import PartitionSpec as P

neg_big = -1e30
epsilon = 1e-06
LANES = 128
bf16 = jnp.bfloat16
f32 = jnp.float32


def xor_blk(x, mask, blocks):
    return lax.ppermute(x, "blk", [(i, i ^ mask) for i in range(blocks)])


def swap_head(x):
    n = lax.axis_size("head")
    return lax.ppermute(x, "head", [(i, n - 1 - i) for i in range(n)])


def gather(x, near, far, blocks, join):
    parts = [x] + [xor_blk(x, f * near, blocks) for f in range(1, far)]
    own = join(parts)
    return [own] + [xor_blk(own, p, blocks) for p in range(1, near)]


def split3(v):
    hi = v.astype(bf16).astype(f32)
    mid = (v - hi).astype(bf16).astype(f32)
    low = (v - hi - mid).astype(bf16).astype(f32)
    return hi, mid, low


def attention_chunk(q, keys, values, scalars, part, near, far, batch, new_tokens, heads_local):
    rows, width = q.shape
    kv_local, ctx_dev, head_dim = keys.shape[1:]
    group = heads_local // kv_local
    slot_rows = rows // batch
    rows_dev = rows // far
    scale = head_dim ** (-0.5) * 1.4426950408889634
    log2e = 1.4426950408889634
    tile = min(512, ctx_dev)

    def kernel(s_ref, q_ref, k_ref, v_ref, o_ref, l_ref):
        slot, g = pl.program_id(0), pl.program_id(1)
        me, own_seq = s_ref[0], s_ref[1]
        seq = own_seq ^ slot
        length = s_ref[2 + seq]
        m_rows = group * slot_rows
        row = lax.broadcasted_iota(jnp.int32, (m_rows, 1), 0) % slot_rows
        piece = row // rows_dev
        first = jnp.zeros((m_rows, 1), jnp.int32)
        for p in range(far // batch):
            mask = (slot * (far // batch) + p) * near + part
            start = ((me ^ mask) * rows_dev) % new_tokens
            first = jnp.where(piece == p, start, first)
        limit = first + row % rows_dev + length - me * ctx_dev
        qb = q_ref[...]
        lhs = jnp.concatenate(
            [qb[:, j * head_dim : (j + 1) * head_dim] for j in range(group)], axis=0
        )
        top = jnp.full((m_rows, 1), neg_big, f32)
        total = jnp.zeros((m_rows, 1), f32)
        acc = jnp.zeros((m_rows, head_dim), f32)
        for t in range(0, ctx_dev, tile):
            s = lax.dot_general(
                lhs, k_ref[0, 0, t : t + tile, :], (((1,), (1,)), ((), ())), preferred_element_type=f32
            )
            pos = lax.broadcasted_iota(jnp.int32, (m_rows, tile), 1) + t
            s = jnp.where(pos <= limit, s, neg_big)
            new_top = jnp.maximum(top, jnp.max(s, axis=1, keepdims=True))
            w = jnp.exp2((s - new_top) * scale)
            fix = jnp.exp2((top - new_top) * scale)
            total = total * fix + jnp.sum(w, axis=1, keepdims=True)
            acc = acc * fix + jnp.dot(
                w.astype(bf16), v_ref[0, 0, t : t + tile, :], preferred_element_type=f32
            )
            top = new_top
        seen = limit >= 0
        mean = acc * jnp.where(seen, 1.0 / total, 0.0)
        lse = jnp.where(seen, top * (scale / log2e) + jnp.log(total), neg_big)
        lane = lax.broadcasted_iota(jnp.int32, (slot_rows, LANES), 1)

        @pl.when(g == 0)
        def _():
            l_ref[...] = jnp.zeros_like(l_ref)

        stats = l_ref[...].astype(f32)
        for j in range(group):
            block = slice(j * slot_rows, (j + 1) * slot_rows)
            o_ref[:, j * head_dim : (j + 1) * head_dim] = mean[block].astype(bf16)
            for i, v in enumerate(split3(lse[block])):
                stats = jnp.where(lane == i * heads_local + g * group + j, v, stats)
        l_ref[...] = stats.astype(bf16)

    return pl.pallas_call(
        kernel,
        grid_spec=pltpu.PrefetchScalarGridSpec(
            num_scalar_prefetch=1,
            grid=(batch, kv_local),
            in_specs=[
                pl.BlockSpec((slot_rows, group * head_dim), lambda i, g, s: (i, g)),
                pl.BlockSpec((1, 1, ctx_dev, head_dim), lambda i, g, s: (s[1] ^ i, g, 0, 0)),
                pl.BlockSpec((1, 1, ctx_dev, head_dim), lambda i, g, s: (s[1] ^ i, g, 0, 0)),
            ],
            out_specs=[
                pl.BlockSpec((slot_rows, group * head_dim), lambda i, g, s: (i, g)),
                pl.BlockSpec((slot_rows, LANES), lambda i, g, s: (i, 0)),
            ],
        ),
        out_shape=[
            jax.ShapeDtypeStruct((rows, width), bf16),
            jax.ShapeDtypeStruct((rows, LANES), bf16),
        ],
        compiler_params=pltpu.CompilerParams(vmem_limit_bytes=24 << 20),
        cost_estimate=pl.CostEstimate(
            flops=4 * rows * width * ctx_dev * 2, bytes_accessed=2 * keys.size * 2, transcendentals=rows * heads_local * ctx_dev
        ),
        name=f"attention_{part}",
    )(scalars, q, keys, values)


def merge(parts, heads_local, head_dim, last):
    rows = parts[0].shape[0]
    width = heads_local * head_dim
    count = len(parts)

    def kernel(*refs):
        ins, out = refs[:count], refs[count]
        lses = []
        for r in ins:
            s = r[:, width:].astype(f32)
            lses.append(
                s + pltpu.roll(s, LANES - heads_local, 1) + pltpu.roll(s, LANES - 2 * heads_local, 1)
            )
        top = functools.reduce(jnp.maximum, lses)
        ws = [jnp.exp(v - top) for v in lses]
        total = functools.reduce(jnp.add, ws)
        ws = [w / total for w in ws]
        for j in range(heads_local):
            cols = slice(j * head_dim, (j + 1) * head_dim)
            acc = sum(w[:, j : j + 1] * r[:, cols].astype(f32) for w, r in zip(ws, ins))
            out[:, cols] = acc.astype(bf16)
        if not last:
            lane = lax.broadcasted_iota(jnp.int32, (rows, LANES), 1)
            hi, mid, low = (
                jnp.where(lane < heads_local, v, 0.0) for v in split3(jnp.where(lane < heads_local, top + jnp.log(total), 0.0))
            )
            out[:, width:] = (
                hi + pltpu.roll(mid, heads_local, 1) + pltpu.roll(low, 2 * heads_local, 1)
            ).astype(bf16)

    return pl.pallas_call(
        kernel,
        out_shape=jax.ShapeDtypeStruct((rows, width if last else width + LANES), bf16),
        compiler_params=pltpu.CompilerParams(vmem_limit_bytes=16 << 20),
        cost_estimate=pl.CostEstimate(flops=rows * width * 1000, bytes_accessed=rows * width * 10, transcendentals=0),
        name=f"merge_{int(last)}",
    )(*parts)


def out_projection(chunks, weight, scalars, near, far, rows_dev):
    count = len(chunks)
    chunk_rows = chunks[0].shape[0]
    rows = count * chunk_rows
    depth, columns = weight.shape
    step = min(1024, depth)

    def kernel(s_ref, *refs):
        ins, w_ref, o_ref, acc = refs[:count], refs[count], refs[count + 1], refs[count + 2]
        k = pl.program_id(0)
        me = s_ref[0]
        there = lax.broadcasted_iota(jnp.int32, (rows, rows), 0)
        here = lax.broadcasted_iota(jnp.int32, (rows, rows), 1)
        piece = here // rows_dev
        mask = (piece % far) * near + piece // far
        goal = (mask ^ me) * rows_dev + here % rows_dev
        order = jnp.where(goal == there, 1.0, 0.0).astype(bf16)
        rel = jnp.concatenate([r[...] for r in ins], axis=0)
        lhs = jnp.dot(order, rel, preferred_element_type=f32).astype(bf16)
        part = jnp.dot(lhs, w_ref[...], preferred_element_type=f32)

        @pl.when(k == 0)
        def _():
            acc[...] = part

        @pl.when(k > 0)
        def _():
            acc[...] += part

        @pl.when(k == pl.num_programs(0) - 1)
        def _():
            o_ref[...] = acc[...].astype(bf16)

    return pl.pallas_call(
        kernel,
        grid_spec=pltpu.PrefetchScalarGridSpec(
            num_scalar_prefetch=1,
            grid=(depth // step,),
            in_specs=[pl.BlockSpec((chunk_rows, step), lambda k, s: (0, k))] * count
            + [pl.BlockSpec((step, columns), lambda k, s: (k, 0))],
            out_specs=pl.BlockSpec((rows, columns), lambda k, s: (0, 0)),
            scratch_shapes=[pltpu.VMEM((rows, columns), f32)],
        ),
        out_shape=jax.ShapeDtypeStruct((rows, columns), bf16),
        compiler_params=pltpu.CompilerParams(vmem_limit_bytes=24 << 20),
        cost_estimate=pl.CostEstimate(flops=2 * rows * depth * columns, bytes_accessed=2 * weight.size, transcendentals=0),
        name="out_projection",
    )(scalars, *chunks, weight)


STAT_ROWS = 8


def stream_step(residual, mine, other, gain, scalars):
    rows, columns = residual.shape
    half = rows // 2

    def kernel(s_ref, r_ref, a_ref, b_ref, g_ref, stream_ref, send_ref):
        core = s_ref[0]
        stream_ref[...] = r_ref[...].astype(f32) + (a_ref[...].astype(f32) + b_ref[...].astype(f32))
        own = stream_ref[pl.ds(pl.multiple_of(core * half, half), half), :]
        send_ref[:half, :] = (own * g_ref[...].astype(f32)).astype(bf16)
        squares = jnp.sum(own * own, axis=1, keepdims=True)
        i = lax.broadcasted_iota(jnp.int32, (half, columns), 0)
        j = lax.broadcasted_iota(jnp.int32, (half, columns), 1)
        line = jnp.sum(jnp.where(i == j, squares, 0.0), axis=0, keepdims=True)
        row = lax.broadcasted_iota(jnp.int32, (STAT_ROWS, columns), 0)
        stats = jnp.zeros((STAT_ROWS, columns), f32)
        for n, v in enumerate(split3(line)):
            stats = jnp.where(row == n, v, stats)
        send_ref[half:, :] = stats.astype(bf16)

    return pl.pallas_call(
        kernel,
        grid_spec=pltpu.PrefetchScalarGridSpec(
            num_scalar_prefetch=1,
            grid=(1,),
            in_specs=[pl.BlockSpec((rows, columns), lambda i, s: (0, 0))] * 3
            + [pl.BlockSpec((1, columns), lambda i, s: (0, 0))],
            out_specs=[
                pl.BlockSpec((rows, columns), lambda i, s: (0, 0)),
                pl.BlockSpec((half + STAT_ROWS, columns), lambda i, s: (0, 0)),
            ],
        ),
        out_shape=[
            jax.ShapeDtypeStruct((rows, columns), f32),
            jax.ShapeDtypeStruct((half + STAT_ROWS, columns), bf16),
        ],
        compiler_params=pltpu.CompilerParams(vmem_limit_bytes=16 << 20),
        name="stream_step",
    )(scalars, residual, mine, other, gain)


def feed_chunk(own, other, gate_weight, up_weight, scalars, carry, part, near, far, width, last):
    half = own.shape[1] - STAT_ROWS
    columns = own.shape[2]
    units = gate_weight.shape[1]
    rows = 2 * half

    def kernel(s_ref, a_ref, b_ref, gw_ref, uw_ref, *rest):
        if carry is not None:
            (gi_ref, ui_ref, si_ref), rest = rest[:3], rest[3:]
        if last:
            h_ref, gate, up, squares = rest
        else:
            gate, up, squares = rest
        k = pl.program_id(0)
        core = s_ref[1]

        @pl.when(k == 0)
        def _():
            if carry is None:
                gate[...] = jnp.zeros_like(gate)
                up[...] = jnp.zeros_like(up)
                squares[...] = jnp.zeros_like(squares)
            else:
                gate[...] = gi_ref[...]
                up[...] = ui_ref[...]
                squares[...] = si_ref[...]

        mine, theirs = a_ref[0], b_ref[0]
        upper = core == 0
        lhs = jnp.concatenate(
            [
                jnp.where(upper, mine[:half].astype(f32), theirs[:half].astype(f32)),
                jnp.where(upper, theirs[:half].astype(f32), mine[:half].astype(f32)),
            ],
            axis=0,
        ).astype(bf16)
        gate[...] += jnp.dot(lhs, gw_ref[...], preferred_element_type=f32)
        up[...] += jnp.dot(lhs, uw_ref[...], preferred_element_type=f32)
        m = jnp.sum(mine[half:].astype(f32), axis=0, keepdims=True)[:, :LANES]
        t = jnp.sum(theirs[half:].astype(f32), axis=0, keepdims=True)[:, :LANES]
        squares[0:1, :] += jnp.where(upper, m, t)
        squares[1:2, :] += jnp.where(upper, t, m)
        if last:

            @pl.when(k == pl.num_programs(0) - 1)
            def _():
                i = lax.broadcasted_iota(jnp.int32, (half, LANES), 0)
                j = lax.broadcasted_iota(jnp.int32, (half, LANES), 1)
                column = jnp.concatenate(
                    [
                        jnp.sum(jnp.where(i == j, squares[n : n + 1, :], 0.0), axis=1, keepdims=True)
                        for n in range(2)
                    ],
                    axis=0,
                )
                r = lax.rsqrt(column / width + epsilon)
                g = gate[...] * r
                u = up[...] * r
                h_ref[...] = (g / (1.0 + jnp.exp(-g)) * u).astype(bf16)

    weight_map = lambda k, s: (s[0] ^ (k * near + part), 0)
    acc_specs = [
        pl.BlockSpec((rows, units), lambda k, s: (0, 0)),
        pl.BlockSpec((rows, units), lambda k, s: (0, 0)),
        pl.BlockSpec((8, LANES), lambda k, s: (0, 0)),
    ]
    acc_shapes = [
        jax.ShapeDtypeStruct((rows, units), f32),
        jax.ShapeDtypeStruct((rows, units), f32),
        jax.ShapeDtypeStruct((8, LANES), f32),
    ]
    scratch = [pltpu.VMEM((rows, units), f32), pltpu.VMEM((rows, units), f32), pltpu.VMEM((8, LANES), f32)]
    return pl.pallas_call(
        kernel,
        grid_spec=pltpu.PrefetchScalarGridSpec(
            num_scalar_prefetch=1,
            grid=(far,),
            in_specs=[
                pl.BlockSpec((1, half + STAT_ROWS, columns), lambda k, s: (k, 0, 0)),
                pl.BlockSpec((1, half + STAT_ROWS, columns), lambda k, s: (k, 0, 0)),
                pl.BlockSpec((columns, units), weight_map),
                pl.BlockSpec((columns, units), weight_map),
            ]
            + (acc_specs if carry is not None else []),
            out_specs=pl.BlockSpec((rows, units), lambda k, s: (0, 0)) if last else acc_specs,
            scratch_shapes=scratch if last else [],
        ),
        out_shape=jax.ShapeDtypeStruct((rows, units), bf16) if last else acc_shapes,
        compiler_params=pltpu.CompilerParams(vmem_limit_bytes=24 << 20),
        cost_estimate=pl.CostEstimate(
            flops=4 * rows * far * columns * units, bytes_accessed=4 * far * columns * units, transcendentals=0
        ),
        name=f"feed_{part}",
    )(scalars, own, other, gate_weight, up_weight, *(carry or ()))


def down_chunk(hidden, weight, scalars, carry, part, near, far, last):
    _, rows, units = hidden.shape
    columns = weight.shape[1]

    def kernel(s_ref, h_ref, w_ref, *rest):
        if carry is not None:
            c_ref, rest = rest[0], rest[1:]
        o_ref, acc = rest if last else (None, rest[0])
        k = pl.program_id(0)

        @pl.when(k == 0)
        def _():
            acc[...] = jnp.zeros_like(acc) if carry is None else c_ref[...]

        acc[...] += jnp.dot(h_ref[0], w_ref[...], preferred_element_type=f32)
        if last:

            @pl.when(k == pl.num_programs(0) - 1)
            def _():
                o_ref[...] = acc[...].astype(bf16)

    whole = pl.BlockSpec((rows, columns), lambda k, s: (0, 0))
    return pl.pallas_call(
        kernel,
        grid_spec=pltpu.PrefetchScalarGridSpec(
            num_scalar_prefetch=1,
            grid=(far,),
            in_specs=[
                pl.BlockSpec((1, rows, units), lambda k, s: (k, 0, 0)),
                pl.BlockSpec((units, columns), lambda k, s: (s[0] ^ (k * near + part), 0)),
            ]
            + ([whole] if carry is not None else []),
            out_specs=whole,
            scratch_shapes=[pltpu.VMEM((rows, columns), f32)] if last else [],
        ),
        out_shape=jax.ShapeDtypeStruct((rows, columns), bf16 if last else f32),
        compiler_params=pltpu.CompilerParams(vmem_limit_bytes=24 << 20),
        cost_estimate=pl.CostEstimate(
            flops=2 * rows * far * columns * units, bytes_accessed=2 * far * columns * units, transcendentals=0
        ),
        name=f"down_{part}",
    )(scalars, hidden, weight, *(() if carry is None else (carry,)))


def body(
    queries,
    key_cache,
    value_cache,
    lengths,
    residual,
    out_weight,
    norm_gain,
    gate_weight,
    up_weight,
    down_weight,
):
    blocks = lax.axis_size("blk")
    me = lax.axis_index("blk").astype(jnp.int32)
    core = lax.axis_index("head").astype(jnp.int32)
    batch, ctx_dev, kv_local, head_dim = key_cache.shape
    rows_dev, width_local = queries.shape
    heads_local = width_local // head_dim
    new_tokens = rows_dev * blocks // batch
    near = 1 << ((blocks.bit_length() - 1) // 2)
    far = blocks // near
    width = residual.shape[1] * blocks

    scalars = jnp.concatenate([jnp.stack([me, me // (blocks // batch)]), lengths])
    spot = jnp.stack([me, core])
    rows_join = lambda parts: jnp.concatenate(parts, axis=0)
    stack_join = lambda parts: jnp.stack(parts, axis=0)

    keys = jnp.transpose(key_cache, (0, 2, 1, 3))
    values = jnp.transpose(value_cache, (0, 2, 1, 3))
    asked = gather(queries, near, far, blocks, rows_join)
    partial = []
    for p in range(near):
        mean, lse = attention_chunk(
            asked[p], keys, values, scalars, p, near, far, batch, new_tokens, heads_local
        )
        both = jnp.concatenate([mean, lse], axis=1)
        partial.append(both if p == 0 else xor_blk(both, p, blocks))
    plane = merge(partial, heads_local, head_dim, False)
    pieces = [plane[f * rows_dev : (f + 1) * rows_dev] for f in range(far)]
    pieces = [pieces[0]] + [xor_blk(pieces[f], f * near, blocks) for f in range(1, far)]
    attn = merge(pieces, heads_local, head_dim, True)

    mine = out_projection(gather(attn, near, far, blocks, rows_join), out_weight, scalars, near, far, rows_dev)
    stream, send = stream_step(residual, mine, swap_head(mine), norm_gain[None, :], core[None])

    normed = gather(send, near, far, blocks, stack_join)
    carry = None
    for p in range(near):
        carry = feed_chunk(
            normed[p], swap_head(normed[p]), gate_weight, up_weight, spot, carry, p, near, far, width, p == near - 1
        )
    hidden = gather(carry, near, far, blocks, stack_join)
    carry = None
    for p in range(near):
        carry = down_chunk(hidden[p], down_weight, spot, carry, p, near, far, p == near - 1)
    total = carry.astype(f32) + swap_head(carry).astype(f32)
    return (stream + total).astype(bf16)


def solution(mesh):
    in_specs = (
        P(("groups", "blk"), "head"),
        P("groups", "blk", "head", None),
        P("groups", "blk", "head", None),
        P("groups"),
        P("groups", "blk"),
        P("head", "blk"),
        P("blk"),
        P(None, ("head", "blk")),
        P(None, ("head", "blk")),
        P("head", "blk"),
    )
    out_specs = P("groups", "blk")
    return jax.shard_map(body, mesh=mesh, in_specs=in_specs, out_specs=out_specs, check_vma=False)
```

```python
import functools

import jax
import jax.numpy as jnp
from jax import lax
from jax.experimental import pallas as pl
from jax.experimental.pallas import tpu as pltpu
from jax.sharding import PartitionSpec as P

neg_big = -1e30
epsilon = 1e-06
LANES = 128
bf16 = jnp.bfloat16
f32 = jnp.float32


def xor_blk(x, mask, blocks):
    return lax.ppermute(x, "blk", [(i, i ^ mask) for i in range(blocks)])


def swap_head(x):
    n = lax.axis_size("head")
    return lax.ppermute(x, "head", [(i, n - 1 - i) for i in range(n)])


def far_parts(x, near, far, blocks):
    return [x] + [xor_blk(x, f * near, blocks) for f in range(1, far)]


def near_parts(own, near, blocks):
    return [own] + [xor_blk(own, p, blocks) for p in range(1, near)]


def gather(x, near, far, blocks, join):
    return near_parts(join(far_parts(x, near, far, blocks)), near, blocks)


def gather_halves(first, second, near, far, blocks, join):
    one = [join(far_parts(first, near, far, blocks))]
    two = [join(far_parts(second, near, far, blocks))]
    for p in range(1, near):
        low, high = p & -p, 1 << (p.bit_length() - 1)
        one.append(xor_blk(one[p ^ low], low, blocks))
        two.append(xor_blk(two[p ^ high], high, blocks))
    return list(zip(one, two))


def split3(v):
    hi = v.astype(bf16).astype(f32)
    mid = (v - hi).astype(bf16).astype(f32)
    low = (v - hi - mid).astype(bf16).astype(f32)
    return hi, mid, low


def attention(qs, parts, keys, values, scalars, near, far, batch, new_tokens, heads_local):
    rows, width = qs[0].shape
    kv_local, ctx_dev, head_dim = keys.shape[1:]
    group = heads_local // kv_local
    slot_rows = rows // batch
    rows_dev = rows // far
    count = len(parts)
    log2e = 1.4426950408889634
    scale = head_dim ** (-0.5) * log2e
    tile = min(512, ctx_dev)
    tiles = ctx_dev // tile
    chunk_m = group * slot_rows
    m_rows = count * chunk_m
    units = batch * kv_local

    def kernel(s_ref, *refs):
        q_refs, k_hbm, v_hbm, o_refs = refs[:count], refs[count], refs[count + 1], refs[count + 2 : -6]
        k_all, v_all, room, best, scores, sems = refs[-6:]
        me = s_ref[0]

        def copies(u, which=(0, 1)):
            slot, g = u // kv_local, u % kv_local
            seq = s_ref[1] ^ slot
            picks = ((k_hbm, k_all), (v_hbm, v_all))
            return [
                pltpu.make_async_copy(picks[i][0].at[seq, g], picks[i][1].at[u], sems.at[u, i]) for i in which
            ]

        for u in range(4):
            for c in copies(u):
                c.start()
        row = lax.broadcasted_iota(jnp.int32, (chunk_m, LANES), 0) % slot_rows
        lanes = lax.broadcasted_iota(jnp.int32, (chunk_m, LANES), 1)
        piece = row // rows_dev
        for slot in range(batch):
            length = s_ref[2 + (s_ref[1] ^ slot)]
            for c, part in enumerate(parts):
                first = jnp.zeros((chunk_m, LANES), jnp.int32)
                for p in range(far // batch):
                    mask = (slot * (far // batch) + p) * near + part
                    start = ((me ^ mask) * rows_dev) % new_tokens
                    first = jnp.where(piece == p, start, first)
                limit = first + row % rows_dev + length - me * ctx_dev
                room[slot, c * chunk_m : (c + 1) * chunk_m, :] = limit - lanes

        def whole(u):
            return s_ref[2 + (s_ref[1] ^ (u // kv_local))] - me * ctx_dev >= ctx_dev - 1

        def produce(u, parity, masked):
            slot, g = u // kv_local, u % kv_local
            own_rows = pl.ds(pl.multiple_of(slot * slot_rows, slot_rows), slot_rows)
            lhs = jnp.concatenate(
                [
                    q[own_rows, pl.ds(pl.multiple_of((g * group + j) * head_dim, head_dim), head_dim)]
                    for q in q_refs
                    for j in range(group)
                ],
                axis=0,
            )
            copies(u, (0,))[0].wait()
            high = jnp.full((m_rows, LANES), neg_big, f32)
            for t in range(tiles):
                s = lax.dot_general(
                    lhs,
                    k_all[u, t * tile : (t + 1) * tile, :],
                    (((1,), (1,)), ((), ())),
                    preferred_element_type=f32,
                )
                for i in range(0, tile, LANES):
                    part = s[:, i : i + LANES]
                    if masked:
                        part = jnp.where(room[slot] >= t * tile + i, part, neg_big)
                    scores[parity, :, t * tile + i : t * tile + i + LANES] = part
                    high = jnp.maximum(high, part)
                yield
            best[parity] = high

        def consume(u, parity):
            slot, g = u // kv_local, u % kv_local
            own_rows = pl.ds(pl.multiple_of(slot * slot_rows, slot_rows), slot_rows)
            top = jnp.max(best[parity], axis=1, keepdims=True)
            copies(u, (1,))[0].wait()
            total = jnp.zeros((m_rows, LANES), f32)
            acc = jnp.zeros((m_rows, head_dim), f32)
            for t in range(tiles):
                w = jnp.exp2((scores[parity, :, t * tile : (t + 1) * tile] - top) * scale)
                for i in range(0, tile, LANES):
                    total += w[:, i : i + LANES]
                acc += jnp.dot(w.astype(bf16), v_all[u, t * tile : (t + 1) * tile, :], preferred_element_type=f32)
                yield
            total = jnp.sum(total, axis=1, keepdims=True)
            seen = top > 0.5 * neg_big
            mean = acc * jnp.where(seen, 1.0 / total, 0.0)
            lse = jnp.where(seen, top * (scale / log2e) + jnp.log(total), neg_big)
            lane = lax.broadcasted_iota(jnp.int32, (slot_rows, LANES), 1)
            for c in range(count):
                stats = o_refs[c][own_rows, width:].astype(f32)
                for j in range(group):
                    block = slice(c * chunk_m + j * slot_rows, c * chunk_m + (j + 1) * slot_rows)
                    head = g * group + j
                    at = pl.ds(pl.multiple_of(head * head_dim, head_dim), head_dim)
                    o_refs[c][own_rows, at] = mean[block].astype(bf16)
                    for i, v in enumerate(split3(lse[block])):
                        stats = jnp.where(lane == i * heads_local + head, v, stats)
                o_refs[c][own_rows, width:] = stats.astype(bf16)

        for o in o_refs:
            o[:, width:] = jnp.zeros((rows, LANES), bf16)

        @pl.when(whole(0))
        def _():
            for _ in produce(0, 0, False):
                pass

        @pl.when(jnp.logical_not(whole(0)))
        def _():
            for _ in produce(0, 0, True):
                pass

        def step(u, nothing):
            @pl.when(u + 4 < units)
            def _():
                for c in copies(u + 4):
                    c.start()

            def both(masked):
                ahead, now = produce(u + 1, (u + 1) % 2, masked), consume(u, u % 2)
                for _ in range(tiles + 1):
                    next(now, None)
                    next(ahead, None)

            @pl.when(whole(u + 1))
            def _():
                both(False)

            @pl.when(jnp.logical_not(whole(u + 1)))
            def _():
                both(True)

            return nothing

        lax.fori_loop(0, units - 1, step, 0)
        for _ in consume(units - 1, (units - 1) % 2):
            pass

    return pl.pallas_call(
        kernel,
        grid_spec=pltpu.PrefetchScalarGridSpec(
            num_scalar_prefetch=1,
            grid=(1,),
            in_specs=[pl.BlockSpec((rows, width), lambda i, s: (0, 0))] * count
            + [pl.BlockSpec(memory_space=pltpu.HBM)] * 2,
            out_specs=[pl.BlockSpec((rows, width + LANES), lambda i, s: (0, 0))] * count,
            scratch_shapes=[
                pltpu.VMEM((units, ctx_dev, head_dim), bf16),
                pltpu.VMEM((units, ctx_dev, head_dim), bf16),
                pltpu.VMEM((batch, m_rows, LANES), jnp.int32),
                pltpu.VMEM((2, m_rows, LANES), f32),
                pltpu.VMEM((2, m_rows, ctx_dev), f32),
                pltpu.SemaphoreType.DMA((units, 2)),
            ],
        ),
        out_shape=[jax.ShapeDtypeStruct((rows, width + LANES), bf16)] * count,
        compiler_params=pltpu.CompilerParams(vmem_limit_bytes=40 << 20),
        cost_estimate=pl.CostEstimate(
            flops=8 * count * rows * width * ctx_dev,
            bytes_accessed=4 * keys.size,
            transcendentals=count * rows * heads_local * ctx_dev,
        ),
    )(scalars, *qs, keys, values)


def merge(parts, heads_local, head_dim, last):
    rows = parts[0].shape[0]
    width = heads_local * head_dim
    count = len(parts)

    def kernel(*refs):
        ins, out = refs[:count], refs[count]
        lses = []
        for r in ins:
            s = r[:, width:].astype(f32)
            lses.append(
                s + pltpu.roll(s, LANES - heads_local, 1) + pltpu.roll(s, LANES - 2 * heads_local, 1)
            )
        top = functools.reduce(jnp.maximum, lses)
        ws = [jnp.exp(v - top) for v in lses]
        total = functools.reduce(jnp.add, ws)
        ws = [w / total for w in ws]
        for j in range(heads_local):
            cols = slice(j * head_dim, (j + 1) * head_dim)
            acc = sum(w[:, j : j + 1] * r[:, cols].astype(f32) for w, r in zip(ws, ins))
            out[:, cols] = acc.astype(bf16)
        if not last:
            lane = lax.broadcasted_iota(jnp.int32, (rows, LANES), 1)
            hi, mid, low = (
                jnp.where(lane < heads_local, v, 0.0) for v in split3(jnp.where(lane < heads_local, top + jnp.log(total), 0.0))
            )
            out[:, width:] = (
                hi + pltpu.roll(mid, heads_local, 1) + pltpu.roll(low, 2 * heads_local, 1)
            ).astype(bf16)

    return pl.pallas_call(
        kernel,
        out_shape=jax.ShapeDtypeStruct((rows, width if last else width + LANES), bf16),
        compiler_params=pltpu.CompilerParams(vmem_limit_bytes=16 << 20),
        cost_estimate=pl.CostEstimate(flops=rows * width * 1000, bytes_accessed=rows * width * 10, transcendentals=0),
    )(*parts)


def out_projection(chunks, weight, scalars, near, far, rows_dev):
    count = len(chunks)
    chunk_rows = chunks[0].shape[0]
    rows = count * chunk_rows
    depth, columns = weight.shape
    step = min(1024, depth)
    steps = depth // step

    def kernel(s_ref, *refs):
        ins, w_hbm, o_ref, w_all, sems = refs[:count], refs[count], refs[count + 1], refs[count + 2], refs[count + 3]
        copies = [
            pltpu.make_async_copy(w_hbm.at[pl.ds(k * step, step)], w_all.at[k], sems.at[k]) for k in range(steps)
        ]
        for c in copies:
            c.start()
        there = lax.broadcasted_iota(jnp.int32, (rows, rows), 0)
        here = lax.broadcasted_iota(jnp.int32, (rows, rows), 1)
        piece = here // rows_dev
        mask = (piece % far) * near + piece // far
        goal = (mask ^ s_ref[0]) * rows_dev + here % rows_dev
        order = jnp.where(goal == there, 1.0, 0.0).astype(bf16)
        acc = jnp.zeros((rows, columns), f32)
        for k in range(steps):
            rel = jnp.concatenate([r[:, k * step : (k + 1) * step] for r in ins], axis=0)
            lhs = jnp.dot(order, rel, preferred_element_type=f32).astype(bf16)
            copies[k].wait()
            acc += jnp.dot(lhs, w_all[k], preferred_element_type=f32)
        o_ref[...] = acc.astype(bf16)

    return pl.pallas_call(
        kernel,
        grid_spec=pltpu.PrefetchScalarGridSpec(
            num_scalar_prefetch=1,
            grid=(1,),
            in_specs=[pl.BlockSpec((chunk_rows, depth), lambda k, s: (0, 0))] * count
            + [pl.BlockSpec(memory_space=pltpu.HBM)],
            out_specs=pl.BlockSpec((rows, columns), lambda k, s: (0, 0)),
            scratch_shapes=[pltpu.VMEM((steps, step, columns), bf16), pltpu.SemaphoreType.DMA((steps,))],
        ),
        out_shape=jax.ShapeDtypeStruct((rows, columns), bf16),
        compiler_params=pltpu.CompilerParams(vmem_limit_bytes=24 << 20),
        cost_estimate=pl.CostEstimate(flops=2 * rows * depth * columns, bytes_accessed=2 * weight.size, transcendentals=0),
        name="out_projection",
    )(scalars, *chunks, weight)


STAT_ROWS = 8


def stream_step(residual, mine, other, gain, scalars):
    rows, columns = residual.shape
    half = rows // 2

    def kernel(s_ref, r_ref, a_ref, b_ref, g_ref, stream_ref, send_ref):
        core = s_ref[0]
        stream_ref[...] = r_ref[...].astype(f32) + (a_ref[...].astype(f32) + b_ref[...].astype(f32))
        own = stream_ref[pl.ds(pl.multiple_of(core * half, half), half), :]
        send_ref[:half, :] = (own * g_ref[...].astype(f32)).astype(bf16)
        squares = jnp.sum(own * own, axis=1, keepdims=True)
        i = lax.broadcasted_iota(jnp.int32, (half, columns), 0)
        j = lax.broadcasted_iota(jnp.int32, (half, columns), 1)
        line = jnp.sum(jnp.where(i == j, squares, 0.0), axis=0, keepdims=True)
        row = lax.broadcasted_iota(jnp.int32, (STAT_ROWS, columns), 0)
        stats = jnp.zeros((STAT_ROWS, columns), f32)
        for n, v in enumerate(split3(line)):
            stats = jnp.where(row == n, v, stats)
        send_ref[half:, :] = stats.astype(bf16)

    return pl.pallas_call(
        kernel,
        grid_spec=pltpu.PrefetchScalarGridSpec(
            num_scalar_prefetch=1,
            grid=(1,),
            in_specs=[pl.BlockSpec((rows, columns), lambda i, s: (0, 0))] * 3
            + [pl.BlockSpec((1, columns), lambda i, s: (0, 0))],
            out_specs=[
                pl.BlockSpec((rows, columns), lambda i, s: (0, 0)),
                pl.BlockSpec((half + STAT_ROWS, columns), lambda i, s: (0, 0)),
            ],
        ),
        out_shape=[
            jax.ShapeDtypeStruct((rows, columns), f32),
            jax.ShapeDtypeStruct((half + STAT_ROWS, columns), bf16),
        ],
        compiler_params=pltpu.CompilerParams(vmem_limit_bytes=16 << 20),
        name="stream_step",
    )(scalars, residual, mine, other, gain)


def feed_chunk(own, other, gate_weight, up_weight, scalars, carry, part, near, far, width, last):
    half = own.shape[1] - STAT_ROWS
    columns = own.shape[2]
    units = gate_weight.shape[1]
    rows = 2 * half

    def kernel(s_ref, a_ref, b_ref, gw_hbm, uw_hbm, *rest):
        g_all, u_all, sems = rest[-3:]
        rest = rest[:-3]
        copies = []
        for k in range(far):
            at = pl.ds(pl.multiple_of((s_ref[0] ^ (k * near + part)) * columns, columns), columns)
            copies.append(
                (
                    pltpu.make_async_copy(gw_hbm.at[at], g_all.at[k], sems.at[k, 0]),
                    pltpu.make_async_copy(uw_hbm.at[at], u_all.at[k], sems.at[k, 1]),
                )
            )
        for pair in copies:
            for c in pair:
                c.start()
        upper = s_ref[1] == 0
        if carry is None:
            gate = jnp.zeros((rows, units), f32)
            up = jnp.zeros((rows, units), f32)
            top = jnp.zeros((1, LANES), f32)
            low = jnp.zeros((1, LANES), f32)
        else:
            gi_ref, ui_ref, si_ref = rest[:3]
            rest = rest[3:]
            gate, up = gi_ref[...], ui_ref[...]
            top, low = si_ref[0:1, :], si_ref[1:2, :]
        for k in range(far):
            mine, theirs = a_ref[k].astype(f32), b_ref[k].astype(f32)
            lhs = jnp.concatenate(
                [
                    jnp.where(upper, mine[:half], theirs[:half]),
                    jnp.where(upper, theirs[:half], mine[:half]),
                ],
                axis=0,
            ).astype(bf16)
            m = jnp.sum(mine[half:], axis=0, keepdims=True)[:, :LANES]
            t = jnp.sum(theirs[half:], axis=0, keepdims=True)[:, :LANES]
            top += jnp.where(upper, m, t)
            low += jnp.where(upper, t, m)
            for c in copies[k]:
                c.wait()
            gate += jnp.dot(lhs, g_all[k], preferred_element_type=f32)
            up += jnp.dot(lhs, u_all[k], preferred_element_type=f32)
        if not last:
            g_ref, u_ref, q_ref = rest
            g_ref[...] = gate
            u_ref[...] = up
            row = lax.broadcasted_iota(jnp.int32, (8, LANES), 0)
            q_ref[...] = jnp.where(row == 0, top, jnp.where(row == 1, low, 0.0))
            return
        i = lax.broadcasted_iota(jnp.int32, (half, LANES), 0)
        j = lax.broadcasted_iota(jnp.int32, (half, LANES), 1)
        for n, line in enumerate((top, low)):
            column = jnp.sum(jnp.where(i == j, line, 0.0), axis=1, keepdims=True)
            r = lax.rsqrt(column / width + epsilon)
            g = gate[n * half : (n + 1) * half] * r
            u = up[n * half : (n + 1) * half] * r
            rest[n][...] = (g / (1.0 + jnp.exp(-g)) * u).astype(bf16)

    flat = lambda shape: pl.BlockSpec(shape, lambda i, s: (0,) * len(shape))
    acc_shapes = [(rows, units), (rows, units), (8, LANES)]
    return pl.pallas_call(
        kernel,
        grid_spec=pltpu.PrefetchScalarGridSpec(
            num_scalar_prefetch=1,
            grid=(1,),
            in_specs=[flat(own.shape), flat(own.shape)]
            + [pl.BlockSpec(memory_space=pltpu.HBM)] * 2
            + ([flat(x) for x in acc_shapes] if carry is not None else []),
            out_specs=[flat((half, units))] * 2 if last else [flat(x) for x in acc_shapes],
            scratch_shapes=[
                pltpu.VMEM((far, columns, units), bf16),
                pltpu.VMEM((far, columns, units), bf16),
                pltpu.SemaphoreType.DMA((far, 2)),
            ],
        ),
        out_shape=[jax.ShapeDtypeStruct((half, units), bf16)] * 2
        if last
        else [jax.ShapeDtypeStruct(x, f32) for x in acc_shapes],
        compiler_params=pltpu.CompilerParams(vmem_limit_bytes=20 << 20),
        cost_estimate=pl.CostEstimate(
            flops=4 * rows * far * columns * units, bytes_accessed=4 * far * columns * units, transcendentals=0
        ),
    )(scalars, own, other, gate_weight, up_weight, *(carry or ()))


def down_chunk(halves, weight, scalars, carry, part, near, far, last):
    _, half, units = halves[0].shape
    rows = half * len(halves)
    columns = weight.shape[1]

    def kernel(s_ref, *refs):
        h_refs, w_hbm, rest = refs[: len(halves)], refs[len(halves)], refs[len(halves) + 1 :]
        w_all, sems = rest[-2:]
        copies = []
        for k in range(far):
            at = pl.ds(pl.multiple_of((s_ref[0] ^ (k * near + part)) * units, units), units)
            copies.append(pltpu.make_async_copy(w_hbm.at[at], w_all.at[k], sems.at[k]))
        for c in copies:
            c.start()
        acc = jnp.zeros((rows, columns), f32) if carry is None else rest[0][...]
        for k in range(far):
            lhs = jnp.concatenate([h[k] for h in h_refs], axis=0)
            copies[k].wait()
            acc += jnp.dot(lhs, w_all[k], preferred_element_type=f32)
        rest[-3][...] = acc.astype(rest[-3].dtype)

    flat = lambda shape: pl.BlockSpec(shape, lambda i, s: (0,) * len(shape))
    return pl.pallas_call(
        kernel,
        grid_spec=pltpu.PrefetchScalarGridSpec(
            num_scalar_prefetch=1,
            grid=(1,),
            in_specs=[flat(h.shape) for h in halves]
            + [pl.BlockSpec(memory_space=pltpu.HBM)]
            + ([flat((rows, columns))] if carry is not None else []),
            out_specs=flat((rows, columns)),
            scratch_shapes=[pltpu.VMEM((far, units, columns), bf16), pltpu.SemaphoreType.DMA((far,))],
        ),
        out_shape=jax.ShapeDtypeStruct((rows, columns), bf16 if last else f32),
        compiler_params=pltpu.CompilerParams(vmem_limit_bytes=20 << 20),
        cost_estimate=pl.CostEstimate(
            flops=2 * rows * far * columns * units, bytes_accessed=2 * far * columns * units, transcendentals=0
        ),
    )(scalars, *halves, weight, *(() if carry is None else (carry,)))


def body(
    queries,
    key_cache,
    value_cache,
    lengths,
    residual,
    out_weight,
    norm_gain,
    gate_weight,
    up_weight,
    down_weight,
):
    blocks = lax.axis_size("blk")
    me = lax.axis_index("blk").astype(jnp.int32)
    core = lax.axis_index("head").astype(jnp.int32)
    batch, _, _, head_dim = key_cache.shape
    rows_dev, width_local = queries.shape
    heads_local = width_local // head_dim
    new_tokens = rows_dev * blocks // batch
    near = 1 << ((blocks.bit_length() - 1) // 2)
    far = blocks // near
    width = residual.shape[1] * blocks

    scalars = jnp.concatenate([jnp.stack([me, me // (blocks // batch)]), lengths])
    spot = jnp.stack([me, core])
    rows_join = lambda parts: jnp.concatenate(parts, axis=0)
    stack_join = lambda parts: jnp.stack(parts, axis=0)

    stay = lambda x: pltpu.with_memory_space_constraint(x, pltpu.HBM)
    out_weight, gate_weight, up_weight, down_weight = map(
        stay, (out_weight, gate_weight, up_weight, down_weight)
    )
    keys = stay(jnp.transpose(key_cache, (0, 2, 1, 3)))
    values = stay(jnp.transpose(value_cache, (0, 2, 1, 3)))
    asked = gather(queries, near, far, blocks, rows_join)
    partial = []
    for group in [[0], list(range(1, near - 1)), [near - 1]]:
        outs = attention(
            [asked[p] for p in group], group, keys, values, scalars, near, far, batch, new_tokens, heads_local
        )
        partial += [o if p == 0 else xor_blk(o, p, blocks) for p, o in zip(group, outs)]
    plane = merge(partial, heads_local, head_dim, False)
    pieces = [plane[f * rows_dev : (f + 1) * rows_dev] for f in range(far)]
    pieces = [pieces[0]] + [xor_blk(pieces[f], f * near, blocks) for f in range(1, far)]
    attn = merge(pieces, heads_local, head_dim, True)

    mine = out_projection(gather(attn, near, far, blocks, rows_join), out_weight, scalars, near, far, rows_dev)
    stream, send = stream_step(residual, mine, swap_head(mine), norm_gain[None, :], core[None])

    normed = gather(send, near, far, blocks, stack_join)
    carry = None
    for p in range(near):
        other = swap_head(normed[p])
        carry = feed_chunk(normed[p], other, gate_weight, up_weight, spot, carry, p, near, far, width, p == near - 1)
    hidden = gather_halves(*carry, near, far, blocks, stack_join)
    carry = None
    for p in range(near):
        carry = down_chunk(hidden[p], down_weight, spot, carry, p, near, far, p == near - 1)
    total = carry.astype(f32) + swap_head(carry).astype(f32)
    return (stream + total).astype(bf16)


def solution(mesh):
    in_specs = (
        P(("groups", "blk"), "head"),
        P("groups", "blk", "head", None),
        P("groups", "blk", "head", None),
        P("groups"),
        P("groups", "blk"),
        P("head", "blk"),
        P("blk"),
        P(None, ("head", "blk")),
        P(None, ("head", "blk")),
        P("head", "blk"),
    )
    out_specs = P("groups", "blk")

    return jax.shard_map(body, mesh=mesh, in_specs=in_specs, out_specs=out_specs, check_vma=False)
```

```python
import functools

import jax
import jax.numpy as jnp
from jax import lax
from jax.experimental import pallas as pl
from jax.experimental.pallas import tpu as pltpu
from jax.sharding import PartitionSpec as P

neg_big = -1e30
epsilon = 1e-06
LANES = 128
bf16 = jnp.bfloat16
f32 = jnp.float32


def xor_blk(x, mask, blocks):
    return lax.ppermute(x, "blk", [(i, i ^ mask) for i in range(blocks)])


def swap_head(x):
    n = lax.axis_size("head")
    return lax.ppermute(x, "head", [(i, n - 1 - i) for i in range(n)])


def far_parts(x, near, far, blocks):
    return [x] + [xor_blk(x, f * near, blocks) for f in range(1, far)]


def near_parts(own, near, blocks):
    return [own] + [xor_blk(own, p, blocks) for p in range(1, near)]


def gather(x, near, far, blocks, join):
    return near_parts(join(far_parts(x, near, far, blocks)), near, blocks)


def gather_halves(first, second, near, far, blocks, join):
    one = [join(far_parts(first, near, far, blocks))]
    two = [join(far_parts(second, near, far, blocks))]
    for p in range(1, near):
        low, high = p & -p, 1 << (p.bit_length() - 1)
        one.append(xor_blk(one[p ^ low], low, blocks))
        two.append(xor_blk(two[p ^ high], high, blocks))
    return list(zip(one, two))


def split3(v):
    hi = v.astype(bf16).astype(f32)
    mid = (v - hi).astype(bf16).astype(f32)
    low = (v - hi - mid).astype(bf16).astype(f32)
    return hi, mid, low


def attention(qs, parts, keys, values, scalars, near, far, batch, new_tokens, heads_local):
    rows, width = qs[0].shape
    kv_local, ctx_dev, head_dim = keys.shape[1:]
    group = heads_local // kv_local
    slot_rows = rows // batch
    rows_dev = rows // far
    count = len(parts)
    log2e = 1.4426950408889634
    scale = head_dim ** (-0.5) * log2e
    tile = min(512, ctx_dev)
    tiles = ctx_dev // tile
    chunk_m = group * slot_rows
    m_rows = count * chunk_m
    units = batch * kv_local

    def kernel(s_ref, *refs):
        q_refs, k_hbm, v_hbm, o_refs = refs[:count], refs[count], refs[count + 1], refs[count + 2 : -6]
        k_all, v_all, room, best, scores, sems = refs[-6:]
        me = s_ref[0]

        def copies(u, which=(0, 1)):
            slot, g = u // kv_local, u % kv_local
            seq = s_ref[1] ^ slot
            picks = ((k_hbm, k_all), (v_hbm, v_all))
            return [
                pltpu.make_async_copy(picks[i][0].at[seq, g], picks[i][1].at[u], sems.at[u, i]) for i in which
            ]

        for u in range(4):
            for c in copies(u):
                c.start()
        row = lax.broadcasted_iota(jnp.int32, (chunk_m, LANES), 0) % slot_rows
        lanes = lax.broadcasted_iota(jnp.int32, (chunk_m, LANES), 1)
        piece = row // rows_dev
        for slot in range(batch):
            length = s_ref[2 + (s_ref[1] ^ slot)]
            for c, part in enumerate(parts):
                first = jnp.zeros((chunk_m, LANES), jnp.int32)
                for p in range(far // batch):
                    mask = (slot * (far // batch) + p) * near + part
                    start = ((me ^ mask) * rows_dev) % new_tokens
                    first = jnp.where(piece == p, start, first)
                limit = first + row % rows_dev + length - me * ctx_dev
                room[slot, c * chunk_m : (c + 1) * chunk_m, :] = limit - lanes

        def whole(u):
            return s_ref[2 + (s_ref[1] ^ (u // kv_local))] - me * ctx_dev >= ctx_dev - 1

        def produce(u, parity, masked):
            slot, g = u // kv_local, u % kv_local
            own_rows = pl.ds(pl.multiple_of(slot * slot_rows, slot_rows), slot_rows)
            lhs = jnp.concatenate(
                [
                    q[own_rows, pl.ds(pl.multiple_of((g * group + j) * head_dim, head_dim), head_dim)]
                    for q in q_refs
                    for j in range(group)
                ],
                axis=0,
            )
            copies(u, (0,))[0].wait()
            high = jnp.full((m_rows, LANES), neg_big, f32)
            for t in range(tiles):
                s = lax.dot_general(
                    lhs,
                    k_all[u, t * tile : (t + 1) * tile, :],
                    (((1,), (1,)), ((), ())),
                    preferred_element_type=f32,
                )
                for i in range(0, tile, LANES):
                    part = s[:, i : i + LANES]
                    if masked:
                        part = jnp.where(room[slot] >= t * tile + i, part, neg_big)
                    scores[parity, :, t * tile + i : t * tile + i + LANES] = part
                    high = jnp.maximum(high, part)
                yield
            best[parity] = high

        def consume(u, parity):
            slot, g = u // kv_local, u % kv_local
            own_rows = pl.ds(pl.multiple_of(slot * slot_rows, slot_rows), slot_rows)
            top = jnp.max(best[parity], axis=1, keepdims=True)
            copies(u, (1,))[0].wait()
            total = jnp.zeros((m_rows, LANES), f32)
            acc = jnp.zeros((m_rows, head_dim), f32)
            for t in range(tiles):
                w = jnp.exp2((scores[parity, :, t * tile : (t + 1) * tile] - top) * scale)
                for i in range(0, tile, LANES):
                    total += w[:, i : i + LANES]
                acc += jnp.dot(w.astype(bf16), v_all[u, t * tile : (t + 1) * tile, :], preferred_element_type=f32)
                yield
            total = jnp.sum(total, axis=1, keepdims=True)
            seen = top > 0.5 * neg_big
            mean = acc * jnp.where(seen, 1.0 / total, 0.0)
            lse = jnp.where(seen, top * (scale / log2e) + jnp.log(total), neg_big)
            lane = lax.broadcasted_iota(jnp.int32, (slot_rows, LANES), 1)
            for c in range(count):
                stats = o_refs[c][own_rows, width:].astype(f32)
                for j in range(group):
                    block = slice(c * chunk_m + j * slot_rows, c * chunk_m + (j + 1) * slot_rows)
                    head = g * group + j
                    at = pl.ds(pl.multiple_of(head * head_dim, head_dim), head_dim)
                    o_refs[c][own_rows, at] = mean[block].astype(bf16)
                    for i, v in enumerate(split3(lse[block])):
                        stats = jnp.where(lane == i * heads_local + head, v, stats)
                o_refs[c][own_rows, width:] = stats.astype(bf16)

        for o in o_refs:
            o[:, width:] = jnp.zeros((rows, LANES), bf16)

        @pl.when(whole(0))
        def _():
            for _ in produce(0, 0, False):
                pass

        @pl.when(jnp.logical_not(whole(0)))
        def _():
            for _ in produce(0, 0, True):
                pass

        def step(u, nothing):
            @pl.when(u + 4 < units)
            def _():
                for c in copies(u + 4):
                    c.start()

            def both(masked):
                ahead, now = produce(u + 1, (u + 1) % 2, masked), consume(u, u % 2)
                for _ in range(tiles + 1):
                    next(now, None)
                    next(ahead, None)

            @pl.when(whole(u + 1))
            def _():
                both(False)

            @pl.when(jnp.logical_not(whole(u + 1)))
            def _():
                both(True)

            return nothing

        lax.fori_loop(0, units - 1, step, 0)
        for _ in consume(units - 1, (units - 1) % 2):
            pass

    return pl.pallas_call(
        kernel,
        grid_spec=pltpu.PrefetchScalarGridSpec(
            num_scalar_prefetch=1,
            grid=(1,),
            in_specs=[pl.BlockSpec((rows, width), lambda i, s: (0, 0))] * count
            + [pl.BlockSpec(memory_space=pltpu.HBM)] * 2,
            out_specs=[pl.BlockSpec((rows, width + LANES), lambda i, s: (0, 0))] * count,
            scratch_shapes=[
                pltpu.VMEM((units, ctx_dev, head_dim), bf16),
                pltpu.VMEM((units, ctx_dev, head_dim), bf16),
                pltpu.VMEM((batch, m_rows, LANES), jnp.int32),
                pltpu.VMEM((2, m_rows, LANES), f32),
                pltpu.VMEM((2, m_rows, ctx_dev), f32),
                pltpu.SemaphoreType.DMA((units, 2)),
            ],
        ),
        out_shape=[jax.ShapeDtypeStruct((rows, width + LANES), bf16)] * count,
        compiler_params=pltpu.CompilerParams(vmem_limit_bytes=40 << 20),
        cost_estimate=pl.CostEstimate(
            flops=8 * count * rows * width * ctx_dev,
            bytes_accessed=4 * keys.size,
            transcendentals=count * rows * heads_local * ctx_dev,
        ),
    )(scalars, *qs, keys, values)


def merge(parts, heads_local, head_dim, last):
    rows = parts[0].shape[0]
    width = heads_local * head_dim
    count = len(parts)

    def kernel(*refs):
        ins, out = refs[:count], refs[count]
        lses = []
        for r in ins:
            s = r[:, width:].astype(f32)
            lses.append(
                s + pltpu.roll(s, LANES - heads_local, 1) + pltpu.roll(s, LANES - 2 * heads_local, 1)
            )
        top = functools.reduce(jnp.maximum, lses)
        ws = [jnp.exp(v - top) for v in lses]
        total = functools.reduce(jnp.add, ws)
        ws = [w / total for w in ws]
        for j in range(heads_local):
            cols = slice(j * head_dim, (j + 1) * head_dim)
            acc = sum(w[:, j : j + 1] * r[:, cols].astype(f32) for w, r in zip(ws, ins))
            out[:, cols] = acc.astype(bf16)
        if not last:
            lane = lax.broadcasted_iota(jnp.int32, (rows, LANES), 1)
            hi, mid, low = (
                jnp.where(lane < heads_local, v, 0.0) for v in split3(jnp.where(lane < heads_local, top + jnp.log(total), 0.0))
            )
            out[:, width:] = (
                hi + pltpu.roll(mid, heads_local, 1) + pltpu.roll(low, 2 * heads_local, 1)
            ).astype(bf16)

    return pl.pallas_call(
        kernel,
        out_shape=jax.ShapeDtypeStruct((rows, width if last else width + LANES), bf16),
        compiler_params=pltpu.CompilerParams(vmem_limit_bytes=16 << 20),
        cost_estimate=pl.CostEstimate(flops=rows * width * 1000, bytes_accessed=rows * width * 10, transcendentals=0),
    )(*parts)


def out_projection(chunks, weight, scalars, near, far, rows_dev):
    count = len(chunks)
    chunk_rows = chunks[0].shape[0]
    rows = count * chunk_rows
    depth, columns = weight.shape
    step = min(1024, depth)
    steps = depth // step

    def kernel(s_ref, *refs):
        ins, w_ref, o_ref = refs[:count], refs[count], refs[count + 1]
        there = lax.broadcasted_iota(jnp.int32, (rows, rows), 0)
        here = lax.broadcasted_iota(jnp.int32, (rows, rows), 1)
        piece = here // rows_dev
        mask = (piece % far) * near + piece // far
        goal = (mask ^ s_ref[0]) * rows_dev + here % rows_dev
        order = jnp.where(goal == there, 1.0, 0.0).astype(bf16)
        acc = jnp.zeros((rows, columns), f32)
        for k in range(steps):
            rel = jnp.concatenate([r[:, k * step : (k + 1) * step] for r in ins], axis=0)
            lhs = jnp.dot(order, rel, preferred_element_type=f32).astype(bf16)
            acc += jnp.dot(lhs, w_ref[k * step : (k + 1) * step, :], preferred_element_type=f32)
        o_ref[...] = acc.astype(bf16)

    return pl.pallas_call(
        kernel,
        grid_spec=pltpu.PrefetchScalarGridSpec(
            num_scalar_prefetch=1,
            grid=(1,),
            in_specs=[pl.BlockSpec((chunk_rows, depth), lambda k, s: (0, 0))] * count
            + [pl.BlockSpec(weight.shape, lambda k, s: (0, 0), pipeline_mode=pl.Buffered(1))],
            out_specs=pl.BlockSpec((rows, columns), lambda k, s: (0, 0)),
        ),
        out_shape=jax.ShapeDtypeStruct((rows, columns), bf16),
        compiler_params=pltpu.CompilerParams(vmem_limit_bytes=24 << 20),
        cost_estimate=pl.CostEstimate(flops=2 * rows * depth * columns, bytes_accessed=2 * weight.size, transcendentals=0),
        name="out_projection",
    )(scalars, *chunks, weight)


STAT_ROWS = 8


def stream_step(residual, mine, other, gain, scalars):
    rows, columns = residual.shape
    half = rows // 2

    def kernel(s_ref, r_ref, a_ref, b_ref, g_ref, stream_ref, send_ref):
        core = s_ref[0]
        stream_ref[...] = r_ref[...].astype(f32) + (a_ref[...].astype(f32) + b_ref[...].astype(f32))
        own = stream_ref[pl.ds(pl.multiple_of(core * half, half), half), :]
        send_ref[:half, :] = (own * g_ref[...].astype(f32)).astype(bf16)
        squares = jnp.sum(own * own, axis=1, keepdims=True)
        i = lax.broadcasted_iota(jnp.int32, (half, columns), 0)
        j = lax.broadcasted_iota(jnp.int32, (half, columns), 1)
        line = jnp.sum(jnp.where(i == j, squares, 0.0), axis=0, keepdims=True)
        row = lax.broadcasted_iota(jnp.int32, (STAT_ROWS, columns), 0)
        stats = jnp.zeros((STAT_ROWS, columns), f32)
        for n, v in enumerate(split3(line)):
            stats = jnp.where(row == n, v, stats)
        send_ref[half:, :] = stats.astype(bf16)

    return pl.pallas_call(
        kernel,
        grid_spec=pltpu.PrefetchScalarGridSpec(
            num_scalar_prefetch=1,
            grid=(1,),
            in_specs=[pl.BlockSpec((rows, columns), lambda i, s: (0, 0))] * 3
            + [pl.BlockSpec((1, columns), lambda i, s: (0, 0))],
            out_specs=[
                pl.BlockSpec((rows, columns), lambda i, s: (0, 0)),
                pl.BlockSpec((half + STAT_ROWS, columns), lambda i, s: (0, 0)),
            ],
        ),
        out_shape=[
            jax.ShapeDtypeStruct((rows, columns), f32),
            jax.ShapeDtypeStruct((half + STAT_ROWS, columns), bf16),
        ],
        compiler_params=pltpu.CompilerParams(vmem_limit_bytes=16 << 20),
        name="stream_step",
    )(scalars, residual, mine, other, gain)


def feed_chunk(own, other, gate_weight, up_weight, scalars, carry, part, near, far, width, last):
    half = own.shape[1] - STAT_ROWS
    columns = own.shape[2]
    units = gate_weight.shape[1]
    rows = 2 * half

    def kernel(s_ref, a_ref, b_ref, gw_hbm, uw_hbm, *rest):
        g_all, u_all, sems = rest[-3:]
        rest = rest[:-3]
        copies = []
        for k in range(far):
            at = pl.ds(pl.multiple_of((s_ref[0] ^ (k * near + part)) * columns, columns), columns)
            copies.append(
                (
                    pltpu.make_async_copy(gw_hbm.at[at], g_all.at[k], sems.at[k, 0]),
                    pltpu.make_async_copy(uw_hbm.at[at], u_all.at[k], sems.at[k, 1]),
                )
            )
        for pair in copies:
            for c in pair:
                c.start()
        upper = s_ref[1] == 0
        if carry is None:
            gate = jnp.zeros((rows, units), f32)
            up = jnp.zeros((rows, units), f32)
            top = jnp.zeros((1, LANES), f32)
            low = jnp.zeros((1, LANES), f32)
        else:
            gi_ref, ui_ref, si_ref = rest[:3]
            rest = rest[3:]
            gate, up = gi_ref[...], ui_ref[...]
            top, low = si_ref[0:1, :], si_ref[1:2, :]
        for k in range(far):
            mine, theirs = a_ref[k].astype(f32), b_ref[k].astype(f32)
            lhs = jnp.concatenate(
                [
                    jnp.where(upper, mine[:half], theirs[:half]),
                    jnp.where(upper, theirs[:half], mine[:half]),
                ],
                axis=0,
            ).astype(bf16)
            m = jnp.sum(mine[half:], axis=0, keepdims=True)[:, :LANES]
            t = jnp.sum(theirs[half:], axis=0, keepdims=True)[:, :LANES]
            top += jnp.where(upper, m, t)
            low += jnp.where(upper, t, m)
            for c in copies[k]:
                c.wait()
            gate += jnp.dot(lhs, g_all[k], preferred_element_type=f32)
            up += jnp.dot(lhs, u_all[k], preferred_element_type=f32)
        if not last:
            g_ref, u_ref, q_ref = rest
            g_ref[...] = gate
            u_ref[...] = up
            row = lax.broadcasted_iota(jnp.int32, (8, LANES), 0)
            q_ref[...] = jnp.where(row == 0, top, jnp.where(row == 1, low, 0.0))
            return
        i = lax.broadcasted_iota(jnp.int32, (half, LANES), 0)
        j = lax.broadcasted_iota(jnp.int32, (half, LANES), 1)
        for n, line in enumerate((top, low)):
            column = jnp.sum(jnp.where(i == j, line, 0.0), axis=1, keepdims=True)
            r = lax.rsqrt(column / width + epsilon)
            g = gate[n * half : (n + 1) * half] * r
            u = up[n * half : (n + 1) * half] * r
            rest[n][...] = (g / (1.0 + jnp.exp(-g)) * u).astype(bf16)

    flat = lambda shape: pl.BlockSpec(shape, lambda i, s: (0,) * len(shape))
    acc_shapes = [(rows, units), (rows, units), (8, LANES)]
    return pl.pallas_call(
        kernel,
        grid_spec=pltpu.PrefetchScalarGridSpec(
            num_scalar_prefetch=1,
            grid=(1,),
            in_specs=[flat(own.shape), flat(own.shape)]
            + [pl.BlockSpec(memory_space=pltpu.HBM)] * 2
            + ([flat(x) for x in acc_shapes] if carry is not None else []),
            out_specs=[flat((half, units))] * 2 if last else [flat(x) for x in acc_shapes],
            scratch_shapes=[
                pltpu.VMEM((far, columns, units), bf16),
                pltpu.VMEM((far, columns, units), bf16),
                pltpu.SemaphoreType.DMA((far, 2)),
            ],
        ),
        out_shape=[jax.ShapeDtypeStruct((half, units), bf16)] * 2
        if last
        else [jax.ShapeDtypeStruct(x, f32) for x in acc_shapes],
        compiler_params=pltpu.CompilerParams(vmem_limit_bytes=20 << 20),
        cost_estimate=pl.CostEstimate(
            flops=4 * rows * far * columns * units, bytes_accessed=4 * far * columns * units, transcendentals=0
        ),
    )(scalars, own, other, gate_weight, up_weight, *(carry or ()))


def down_chunk(halves, weight, scalars, carry, part, near, far, last):
    _, half, units = halves[0].shape
    rows = half * len(halves)
    columns = weight.shape[1]

    def kernel(s_ref, *refs):
        h_refs, w_ref, rest = refs[: len(halves)], refs[len(halves)], refs[len(halves) + 1 :]
        acc = jnp.zeros((rows, columns), f32) if carry is None else rest[0][...]
        for k in range(far):
            lhs = jnp.concatenate([h[k] for h in h_refs], axis=0)
            at = pl.ds(pl.multiple_of((s_ref[0] ^ (k * near + part)) * units, units), units)
            acc += jnp.dot(lhs, w_ref[at, :], preferred_element_type=f32)
        rest[-1][...] = acc.astype(rest[-1].dtype)

    flat = lambda shape: pl.BlockSpec(shape, lambda i, s: (0,) * len(shape))
    return pl.pallas_call(
        kernel,
        grid_spec=pltpu.PrefetchScalarGridSpec(
            num_scalar_prefetch=1,
            grid=(1,),
            in_specs=[flat(h.shape) for h in halves]
            + [pl.BlockSpec(weight.shape, lambda i, s: (0, 0), pipeline_mode=pl.Buffered(1))]
            + ([flat((rows, columns))] if carry is not None else []),
            out_specs=flat((rows, columns)),
        ),
        out_shape=jax.ShapeDtypeStruct((rows, columns), bf16 if last else f32),
        compiler_params=pltpu.CompilerParams(vmem_limit_bytes=20 << 20),
        cost_estimate=pl.CostEstimate(
            flops=2 * rows * far * columns * units, bytes_accessed=2 * far * columns * units, transcendentals=0
        ),
    )(scalars, *halves, weight, *(() if carry is None else (carry,)))


def body(
    queries,
    key_cache,
    value_cache,
    lengths,
    residual,
    out_weight,
    norm_gain,
    gate_weight,
    up_weight,
    down_weight,
):
    blocks = lax.axis_size("blk")
    me = lax.axis_index("blk").astype(jnp.int32)
    core = lax.axis_index("head").astype(jnp.int32)
    batch, _, _, head_dim = key_cache.shape
    rows_dev, width_local = queries.shape
    heads_local = width_local // head_dim
    new_tokens = rows_dev * blocks // batch
    near = 1 << ((blocks.bit_length() - 1) // 2)
    far = blocks // near
    width = residual.shape[1] * blocks

    scalars = jnp.concatenate([jnp.stack([me, me // (blocks // batch)]), lengths])
    spot = jnp.stack([me, core])
    rows_join = lambda parts: jnp.concatenate(parts, axis=0)
    stack_join = lambda parts: jnp.stack(parts, axis=0)

    stay = lambda x: pltpu.with_memory_space_constraint(x, pltpu.HBM)
    gate_weight, up_weight = stay(gate_weight), stay(up_weight)
    keys = stay(jnp.transpose(key_cache, (0, 2, 1, 3)))
    values = stay(jnp.transpose(value_cache, (0, 2, 1, 3)))
    asked = gather(queries, near, far, blocks, rows_join)
    partial = []
    for group in [[0], list(range(1, near - 1)), [near - 1]]:
        outs = attention(
            [asked[p] for p in group], group, keys, values, scalars, near, far, batch, new_tokens, heads_local
        )
        partial += [o if p == 0 else xor_blk(o, p, blocks) for p, o in zip(group, outs)]
    plane = merge(partial, heads_local, head_dim, False)
    pieces = [plane[f * rows_dev : (f + 1) * rows_dev] for f in range(far)]
    pieces = [pieces[0]] + [xor_blk(pieces[f], f * near, blocks) for f in range(1, far)]
    attn = merge(pieces, heads_local, head_dim, True)

    mine = out_projection(gather(attn, near, far, blocks, rows_join), out_weight, scalars, near, far, rows_dev)
    stream, send = stream_step(residual, mine, swap_head(mine), norm_gain[None, :], core[None])

    normed = gather(send, near, far, blocks, stack_join)
    carry = None
    for p in range(near):
        other = swap_head(normed[p])
        carry = feed_chunk(normed[p], other, gate_weight, up_weight, spot, carry, p, near, far, width, p == near - 1)
    hidden = gather_halves(*carry, near, far, blocks, stack_join)
    carry = None
    for p in range(near):
        carry = down_chunk(hidden[p], down_weight, spot, carry, p, near, far, p == near - 1)
    total = carry.astype(f32) + swap_head(carry).astype(f32)
    return (stream + total).astype(bf16)


def solution(mesh):
    in_specs = (
        P(("groups", "blk"), "head"),
        P("groups", "blk", "head", None),
        P("groups", "blk", "head", None),
        P("groups"),
        P("groups", "blk"),
        P("head", "blk"),
        P("blk"),
        P(None, ("head", "blk")),
        P(None, ("head", "blk")),
        P("head", "blk"),
    )
    out_specs = P("groups", "blk")

    return jax.shard_map(body, mesh=mesh, in_specs=in_specs, out_specs=out_specs, check_vma=False)
```

```python
import functools

import jax
import jax.numpy as jnp
from jax import lax
from jax.experimental import pallas as pl
from jax.experimental.pallas import tpu as pltpu
from jax.sharding import PartitionSpec as P

neg_big = -1e30
epsilon = 1e-06
LANES = 128
bf16 = jnp.bfloat16
f32 = jnp.float32


def xor_blk(x, mask, blocks):
    return lax.ppermute(x, "blk", [(i, i ^ mask) for i in range(blocks)])


def swap_head(x):
    n = lax.axis_size("head")
    return lax.ppermute(x, "head", [(i, n - 1 - i) for i in range(n)])


def far_parts(x, near, far, blocks):
    return [x] + [xor_blk(x, f * near, blocks) for f in range(1, far)]


def near_parts(own, near, blocks):
    return [own] + [xor_blk(own, p, blocks) for p in range(1, near)]


def gather(x, near, far, blocks, join):
    return near_parts(join(far_parts(x, near, far, blocks)), near, blocks)


def gather_halves(first, second, near, far, blocks, join):
    one = [join(far_parts(first, near, far, blocks))]
    two = [join(far_parts(second, near, far, blocks))]
    for p in range(1, near):
        low, high = p & -p, 1 << (p.bit_length() - 1)
        one.append(xor_blk(one[p ^ low], low, blocks))
        two.append(xor_blk(two[p ^ high], high, blocks))
    return list(zip(one, two))


def split3(v):
    hi = v.astype(bf16).astype(f32)
    mid = (v - hi).astype(bf16).astype(f32)
    low = (v - hi - mid).astype(bf16).astype(f32)
    return hi, mid, low


def attention(qs, parts, keys, values, scalars, near, far, batch, new_tokens, heads_local):
    rows, width = qs[0].shape
    kv_local, ctx_dev, head_dim = keys.shape[1:]
    group = heads_local // kv_local
    slot_rows = rows // batch
    rows_dev = rows // far
    count = len(parts)
    log2e = 1.4426950408889634
    scale = head_dim ** (-0.5) * log2e
    tile = min(512, ctx_dev)
    tiles = ctx_dev // tile
    chunk_m = group * slot_rows
    m_rows = count * chunk_m
    units = batch * kv_local

    def kernel(s_ref, *refs):
        q_refs, k_hbm, v_hbm, o_refs = refs[:count], refs[count], refs[count + 1], refs[count + 2 : -6]
        k_all, v_all, room, best, scores, sems = refs[-6:]
        me = s_ref[0]

        def copies(u, which=(0, 1)):
            slot, g = u // kv_local, u % kv_local
            seq = s_ref[1] ^ slot
            picks = ((k_hbm, k_all), (v_hbm, v_all))
            return [
                pltpu.make_async_copy(picks[i][0].at[seq, g], picks[i][1].at[u], sems.at[u, i]) for i in which
            ]

        for u in range(4):
            for c in copies(u):
                c.start()
        row = lax.broadcasted_iota(jnp.int32, (chunk_m, LANES), 0) % slot_rows
        lanes = lax.broadcasted_iota(jnp.int32, (chunk_m, LANES), 1)
        piece = row // rows_dev
        for slot in range(batch):
            length = s_ref[2 + (s_ref[1] ^ slot)]
            for c, part in enumerate(parts):
                first = jnp.zeros((chunk_m, LANES), jnp.int32)
                for p in range(far // batch):
                    mask = (slot * (far // batch) + p) * near + part
                    start = ((me ^ mask) * rows_dev) % new_tokens
                    first = jnp.where(piece == p, start, first)
                limit = first + row % rows_dev + length - me * ctx_dev
                room[slot, c * chunk_m : (c + 1) * chunk_m, :] = limit - lanes

        def whole(u):
            return s_ref[2 + (s_ref[1] ^ (u // kv_local))] - me * ctx_dev >= ctx_dev - 1

        def produce(u, parity, masked):
            slot, g = u // kv_local, u % kv_local
            own_rows = pl.ds(pl.multiple_of(slot * slot_rows, slot_rows), slot_rows)
            lhs = jnp.concatenate(
                [
                    q[own_rows, pl.ds(pl.multiple_of((g * group + j) * head_dim, head_dim), head_dim)]
                    for q in q_refs
                    for j in range(group)
                ],
                axis=0,
            )
            copies(u, (0,))[0].wait()
            high = jnp.full((m_rows, LANES), neg_big, f32)
            for t in range(tiles):
                s = lax.dot_general(
                    lhs,
                    k_all[u, t * tile : (t + 1) * tile, :],
                    (((1,), (1,)), ((), ())),
                    preferred_element_type=f32,
                )
                for i in range(0, tile, LANES):
                    part = s[:, i : i + LANES]
                    if masked:
                        part = jnp.where(room[slot] >= t * tile + i, part, neg_big)
                    scores[parity, :, t * tile + i : t * tile + i + LANES] = part
                    high = jnp.maximum(high, part)
                yield
            best[parity] = high

        def consume(u, parity):
            slot, g = u // kv_local, u % kv_local
            own_rows = pl.ds(pl.multiple_of(slot * slot_rows, slot_rows), slot_rows)
            top = jnp.max(best[parity], axis=1, keepdims=True)
            copies(u, (1,))[0].wait()
            total = jnp.zeros((m_rows, LANES), f32)
            acc = jnp.zeros((m_rows, head_dim), f32)
            for t in range(tiles):
                w = jnp.exp2((scores[parity, :, t * tile : (t + 1) * tile] - top) * scale)
                for i in range(0, tile, LANES):
                    total += w[:, i : i + LANES]
                acc += jnp.dot(w.astype(bf16), v_all[u, t * tile : (t + 1) * tile, :], preferred_element_type=f32)
                yield
            total = jnp.sum(total, axis=1, keepdims=True)
            seen = top > 0.5 * neg_big
            mean = acc * jnp.where(seen, 1.0 / total, 0.0)
            lse = jnp.where(seen, top * (scale / log2e) + jnp.log(total), neg_big)
            lane = lax.broadcasted_iota(jnp.int32, (slot_rows, LANES), 1)
            for c in range(count):
                stats = o_refs[c][own_rows, width:].astype(f32)
                for j in range(group):
                    block = slice(c * chunk_m + j * slot_rows, c * chunk_m + (j + 1) * slot_rows)
                    head = g * group + j
                    at = pl.ds(pl.multiple_of(head * head_dim, head_dim), head_dim)
                    o_refs[c][own_rows, at] = mean[block].astype(bf16)
                    for i, v in enumerate(split3(lse[block])):
                        stats = jnp.where(lane == i * heads_local + head, v, stats)
                o_refs[c][own_rows, width:] = stats.astype(bf16)

        for o in o_refs:
            o[:, width:] = jnp.zeros((rows, LANES), bf16)

        @pl.when(whole(0))
        def _():
            for _ in produce(0, 0, False):
                pass

        @pl.when(jnp.logical_not(whole(0)))
        def _():
            for _ in produce(0, 0, True):
                pass

        def step(u, nothing):
            @pl.when(u + 4 < units)
            def _():
                for c in copies(u + 4):
                    c.start()

            def both(masked):
                ahead, now = produce(u + 1, (u + 1) % 2, masked), consume(u, u % 2)
                for _ in range(tiles + 1):
                    next(now, None)
                    next(ahead, None)

            @pl.when(whole(u + 1))
            def _():
                both(False)

            @pl.when(jnp.logical_not(whole(u + 1)))
            def _():
                both(True)

            return nothing

        lax.fori_loop(0, units - 1, step, 0)
        for _ in consume(units - 1, (units - 1) % 2):
            pass

    return pl.pallas_call(
        kernel,
        grid_spec=pltpu.PrefetchScalarGridSpec(
            num_scalar_prefetch=1,
            grid=(1,),
            in_specs=[pl.BlockSpec((rows, width), lambda i, s: (0, 0))] * count
            + [pl.BlockSpec(memory_space=pltpu.HBM)] * 2,
            out_specs=[pl.BlockSpec((rows, width + LANES), lambda i, s: (0, 0))] * count,
            scratch_shapes=[
                pltpu.VMEM((units, ctx_dev, head_dim), bf16),
                pltpu.VMEM((units, ctx_dev, head_dim), bf16),
                pltpu.VMEM((batch, m_rows, LANES), jnp.int32),
                pltpu.VMEM((2, m_rows, LANES), f32),
                pltpu.VMEM((2, m_rows, ctx_dev), f32),
                pltpu.SemaphoreType.DMA((units, 2)),
            ],
        ),
        out_shape=[jax.ShapeDtypeStruct((rows, width + LANES), bf16)] * count,
        compiler_params=pltpu.CompilerParams(vmem_limit_bytes=40 << 20),
        cost_estimate=pl.CostEstimate(
            flops=8 * count * rows * width * ctx_dev,
            bytes_accessed=4 * keys.size,
            transcendentals=count * rows * heads_local * ctx_dev,
        ),
    )(scalars, *qs, keys, values)


def merge(parts, heads_local, head_dim, last):
    rows = parts[0].shape[0]
    width = heads_local * head_dim
    count = len(parts)

    def kernel(*refs):
        ins, out = refs[:count], refs[count]
        lses = []
        for r in ins:
            s = r[:, width:].astype(f32)
            lses.append(
                s + pltpu.roll(s, LANES - heads_local, 1) + pltpu.roll(s, LANES - 2 * heads_local, 1)
            )
        top = functools.reduce(jnp.maximum, lses)
        ws = [jnp.exp(v - top) for v in lses]
        total = functools.reduce(jnp.add, ws)
        ws = [w / total for w in ws]
        for j in range(heads_local):
            cols = slice(j * head_dim, (j + 1) * head_dim)
            acc = sum(w[:, j : j + 1] * r[:, cols].astype(f32) for w, r in zip(ws, ins))
            out[:, cols] = acc.astype(bf16)
        if not last:
            lane = lax.broadcasted_iota(jnp.int32, (rows, LANES), 1)
            hi, mid, low = (
                jnp.where(lane < heads_local, v, 0.0) for v in split3(jnp.where(lane < heads_local, top + jnp.log(total), 0.0))
            )
            out[:, width:] = (
                hi + pltpu.roll(mid, heads_local, 1) + pltpu.roll(low, 2 * heads_local, 1)
            ).astype(bf16)

    return pl.pallas_call(
        kernel,
        out_shape=jax.ShapeDtypeStruct((rows, width if last else width + LANES), bf16),
        compiler_params=pltpu.CompilerParams(vmem_limit_bytes=16 << 20),
        cost_estimate=pl.CostEstimate(flops=rows * width * 1000, bytes_accessed=rows * width * 10, transcendentals=0),
    )(*parts)


def out_projection(chunks, weight, scalars, near, far, rows_dev):
    count = len(chunks)
    chunk_rows = chunks[0].shape[0]
    rows = count * chunk_rows
    depth, columns = weight.shape
    step = min(1024, depth)
    steps = depth // step

    def kernel(s_ref, *refs):
        ins, w_ref, o_ref = refs[:count], refs[count], refs[count + 1]
        there = lax.broadcasted_iota(jnp.int32, (rows, rows), 0)
        here = lax.broadcasted_iota(jnp.int32, (rows, rows), 1)
        piece = here // rows_dev
        mask = (piece % far) * near + piece // far
        goal = (mask ^ s_ref[0]) * rows_dev + here % rows_dev
        order = jnp.where(goal == there, 1.0, 0.0).astype(bf16)
        acc = jnp.zeros((rows, columns), f32)
        for k in range(steps):
            rel = jnp.concatenate([r[:, k * step : (k + 1) * step] for r in ins], axis=0)
            lhs = jnp.dot(order, rel, preferred_element_type=f32).astype(bf16)
            acc += jnp.dot(lhs, w_ref[k * step : (k + 1) * step, :], preferred_element_type=f32)
        o_ref[...] = acc.astype(bf16)

    return pl.pallas_call(
        kernel,
        grid_spec=pltpu.PrefetchScalarGridSpec(
            num_scalar_prefetch=1,
            grid=(1,),
            in_specs=[pl.BlockSpec((chunk_rows, depth), lambda k, s: (0, 0))] * count
            + [pl.BlockSpec(weight.shape, lambda k, s: (0, 0), pipeline_mode=pl.Buffered(1))],
            out_specs=pl.BlockSpec((rows, columns), lambda k, s: (0, 0)),
        ),
        out_shape=jax.ShapeDtypeStruct((rows, columns), bf16),
        compiler_params=pltpu.CompilerParams(vmem_limit_bytes=24 << 20),
        cost_estimate=pl.CostEstimate(flops=2 * rows * depth * columns, bytes_accessed=2 * weight.size, transcendentals=0),
        name="out_projection",
    )(scalars, *chunks, weight)


STAT_ROWS = 8


def stream_step(residual, mine, other, gain, scalars):
    rows, columns = residual.shape
    half = rows // 2

    def kernel(s_ref, r_ref, a_ref, b_ref, g_ref, stream_ref, send_ref):
        core = s_ref[0]
        stream_ref[...] = r_ref[...].astype(f32) + (a_ref[...].astype(f32) + b_ref[...].astype(f32))
        own = stream_ref[pl.ds(pl.multiple_of(core * half, half), half), :]
        send_ref[:half, :] = (own * g_ref[...].astype(f32)).astype(bf16)
        squares = jnp.sum(own * own, axis=1, keepdims=True)
        i = lax.broadcasted_iota(jnp.int32, (half, columns), 0)
        j = lax.broadcasted_iota(jnp.int32, (half, columns), 1)
        line = jnp.sum(jnp.where(i == j, squares, 0.0), axis=0, keepdims=True)
        row = lax.broadcasted_iota(jnp.int32, (STAT_ROWS, columns), 0)
        stats = jnp.zeros((STAT_ROWS, columns), f32)
        for n, v in enumerate(split3(line)):
            stats = jnp.where(row == n, v, stats)
        send_ref[half:, :] = stats.astype(bf16)

    return pl.pallas_call(
        kernel,
        grid_spec=pltpu.PrefetchScalarGridSpec(
            num_scalar_prefetch=1,
            grid=(1,),
            in_specs=[pl.BlockSpec((rows, columns), lambda i, s: (0, 0))] * 3
            + [pl.BlockSpec((1, columns), lambda i, s: (0, 0))],
            out_specs=[
                pl.BlockSpec((rows, columns), lambda i, s: (0, 0)),
                pl.BlockSpec((half + STAT_ROWS, columns), lambda i, s: (0, 0)),
            ],
        ),
        out_shape=[
            jax.ShapeDtypeStruct((rows, columns), f32),
            jax.ShapeDtypeStruct((half + STAT_ROWS, columns), bf16),
        ],
        compiler_params=pltpu.CompilerParams(vmem_limit_bytes=16 << 20),
        name="stream_step",
    )(scalars, residual, mine, other, gain)


def feed_chunk(own, other, gate_weight, up_weight, scalars, carry, part, near, far, width, last, staged):
    half = own.shape[1] - STAT_ROWS
    columns = own.shape[2]
    units = gate_weight.shape[-1]
    rows = 2 * half

    def kernel(s_ref, a_ref, b_ref, gw_hbm, uw_hbm, *rest):
        copies = []
        if staged:
            g_all, u_all = gw_hbm, uw_hbm
        else:
            g_all, u_all, sems = rest[-3:]
            rest = rest[:-3]
            for k in range(far):
                at = pl.ds(pl.multiple_of((s_ref[0] ^ (k * near + part)) * columns, columns), columns)
                copies.append(
                    (
                        pltpu.make_async_copy(gw_hbm.at[at], g_all.at[k], sems.at[k, 0]),
                        pltpu.make_async_copy(uw_hbm.at[at], u_all.at[k], sems.at[k, 1]),
                    )
                )
        for pair in copies:
            for c in pair:
                c.start()
        upper = s_ref[1] == 0
        if carry is None:
            gate = jnp.zeros((rows, units), f32)
            up = jnp.zeros((rows, units), f32)
            top = jnp.zeros((1, LANES), f32)
            low = jnp.zeros((1, LANES), f32)
        else:
            gi_ref, ui_ref, si_ref = rest[:3]
            rest = rest[3:]
            gate, up = gi_ref[...], ui_ref[...]
            top, low = si_ref[0:1, :], si_ref[1:2, :]
        for k in range(far):
            mine, theirs = a_ref[k].astype(f32), b_ref[k].astype(f32)
            lhs = jnp.concatenate(
                [
                    jnp.where(upper, mine[:half], theirs[:half]),
                    jnp.where(upper, theirs[:half], mine[:half]),
                ],
                axis=0,
            ).astype(bf16)
            m = jnp.sum(mine[half:], axis=0, keepdims=True)[:, :LANES]
            t = jnp.sum(theirs[half:], axis=0, keepdims=True)[:, :LANES]
            top += jnp.where(upper, m, t)
            low += jnp.where(upper, t, m)
            for c in copies[k] if copies else ():
                c.wait()
            gate += jnp.dot(lhs, g_all[k], preferred_element_type=f32)
            up += jnp.dot(lhs, u_all[k], preferred_element_type=f32)
        if not last:
            g_ref, u_ref, q_ref = rest
            g_ref[...] = gate
            u_ref[...] = up
            row = lax.broadcasted_iota(jnp.int32, (8, LANES), 0)
            q_ref[...] = jnp.where(row == 0, top, jnp.where(row == 1, low, 0.0))
            return
        i = lax.broadcasted_iota(jnp.int32, (half, LANES), 0)
        j = lax.broadcasted_iota(jnp.int32, (half, LANES), 1)
        for n, line in enumerate((top, low)):
            column = jnp.sum(jnp.where(i == j, line, 0.0), axis=1, keepdims=True)
            r = lax.rsqrt(column / width + epsilon)
            g = gate[n * half : (n + 1) * half] * r
            u = up[n * half : (n + 1) * half] * r
            rest[n][...] = (g / (1.0 + jnp.exp(-g)) * u).astype(bf16)

    flat = lambda shape: pl.BlockSpec(shape, lambda i, s: (0,) * len(shape))
    acc_shapes = [(rows, units), (rows, units), (8, LANES)]
    return pl.pallas_call(
        kernel,
        grid_spec=pltpu.PrefetchScalarGridSpec(
            num_scalar_prefetch=1,
            grid=(1,),
            in_specs=[flat(own.shape), flat(own.shape)]
            + (
                [pl.BlockSpec(gate_weight.shape, lambda i, s: (0, 0, 0), pipeline_mode=pl.Buffered(1))]
                if staged
                else [pl.BlockSpec(memory_space=pltpu.HBM)]
            )
            * 2
            + ([flat(x) for x in acc_shapes] if carry is not None else []),
            out_specs=[flat((half, units))] * 2 if last else [flat(x) for x in acc_shapes],
            scratch_shapes=[]
            if staged
            else [
                pltpu.VMEM((far, columns, units), bf16),
                pltpu.VMEM((far, columns, units), bf16),
                pltpu.SemaphoreType.DMA((far, 2)),
            ],
        ),
        out_shape=[jax.ShapeDtypeStruct((half, units), bf16)] * 2
        if last
        else [jax.ShapeDtypeStruct(x, f32) for x in acc_shapes],
        compiler_params=pltpu.CompilerParams(vmem_limit_bytes=20 << 20),
        cost_estimate=pl.CostEstimate(
            flops=4 * rows * far * columns * units, bytes_accessed=4 * far * columns * units, transcendentals=0
        ),
    )(scalars, own, other, gate_weight, up_weight, *(carry or ()))


def bring(gate_weight, up_weight, scalars, columns, part, near, far):
    units = gate_weight.shape[1]

    def kernel(s_ref, gw_hbm, uw_hbm, g_ref, u_ref, sems):
        copies = []
        for k in range(far):
            at = pl.ds(pl.multiple_of((s_ref[0] ^ (k * near + part)) * columns, columns), columns)
            copies.append(pltpu.make_async_copy(gw_hbm.at[at], g_ref.at[k], sems.at[k, 0]))
            copies.append(pltpu.make_async_copy(uw_hbm.at[at], u_ref.at[k], sems.at[k, 1]))
        for c in copies:
            c.start()
        for c in copies:
            c.wait()

    shape = (far, columns, units)
    return pl.pallas_call(
        kernel,
        grid_spec=pltpu.PrefetchScalarGridSpec(
            num_scalar_prefetch=1,
            grid=(1,),
            in_specs=[pl.BlockSpec(memory_space=pltpu.HBM)] * 2,
            out_specs=[pl.BlockSpec(shape, lambda i, s: (0, 0, 0), pipeline_mode=pl.Buffered(1))] * 2,
            scratch_shapes=[pltpu.SemaphoreType.DMA((far, 2))],
        ),
        out_shape=[jax.ShapeDtypeStruct(shape, bf16)] * 2,
        compiler_params=pltpu.CompilerParams(vmem_limit_bytes=16 << 20),
        cost_estimate=pl.CostEstimate(flops=4000000000, bytes_accessed=8 * far * columns * units, transcendentals=0),
    )(scalars, gate_weight, up_weight)


def down_chunk(halves, weight, scalars, carry, part, near, far, last):
    _, half, units = halves[0].shape
    rows = half * len(halves)
    columns = weight.shape[1]

    def kernel(s_ref, *refs):
        h_refs, w_ref, rest = refs[: len(halves)], refs[len(halves)], refs[len(halves) + 1 :]
        acc = jnp.zeros((rows, columns), f32) if carry is None else rest[0][...]
        for k in range(far):
            lhs = jnp.concatenate([h[k] for h in h_refs], axis=0)
            at = pl.ds(pl.multiple_of((s_ref[0] ^ (k * near + part)) * units, units), units)
            acc += jnp.dot(lhs, w_ref[at, :], preferred_element_type=f32)
        rest[-1][...] = acc.astype(rest[-1].dtype)

    flat = lambda shape: pl.BlockSpec(shape, lambda i, s: (0,) * len(shape))
    return pl.pallas_call(
        kernel,
        grid_spec=pltpu.PrefetchScalarGridSpec(
            num_scalar_prefetch=1,
            grid=(1,),
            in_specs=[flat(h.shape) for h in halves]
            + [pl.BlockSpec(weight.shape, lambda i, s: (0, 0), pipeline_mode=pl.Buffered(1))]
            + ([flat((rows, columns))] if carry is not None else []),
            out_specs=flat((rows, columns)),
        ),
        out_shape=jax.ShapeDtypeStruct((rows, columns), bf16 if last else f32),
        compiler_params=pltpu.CompilerParams(vmem_limit_bytes=20 << 20),
        cost_estimate=pl.CostEstimate(
            flops=2 * rows * far * columns * units, bytes_accessed=2 * far * columns * units, transcendentals=0
        ),
    )(scalars, *halves, weight, *(() if carry is None else (carry,)))


def body(
    queries,
    key_cache,
    value_cache,
    lengths,
    residual,
    out_weight,
    norm_gain,
    gate_weight,
    up_weight,
    down_weight,
):
    blocks = lax.axis_size("blk")
    me = lax.axis_index("blk").astype(jnp.int32)
    core = lax.axis_index("head").astype(jnp.int32)
    batch, _, _, head_dim = key_cache.shape
    rows_dev, width_local = queries.shape
    heads_local = width_local // head_dim
    new_tokens = rows_dev * blocks // batch
    near = 1 << ((blocks.bit_length() - 1) // 2)
    far = blocks // near
    width = residual.shape[1] * blocks

    scalars = jnp.concatenate([jnp.stack([me, me // (blocks // batch)]), lengths])
    spot = jnp.stack([me, core])
    rows_join = lambda parts: jnp.concatenate(parts, axis=0)
    stack_join = lambda parts: jnp.stack(parts, axis=0)

    stay = lambda x: pltpu.with_memory_space_constraint(x, pltpu.HBM)
    gate_weight, up_weight = stay(gate_weight), stay(up_weight)
    keys = stay(jnp.transpose(key_cache, (0, 2, 1, 3)))
    values = stay(jnp.transpose(value_cache, (0, 2, 1, 3)))
    asked = gather(queries, near, far, blocks, rows_join)
    partial = []
    for group in [[0], list(range(1, near - 1)), [near - 1]]:
        outs = attention(
            [asked[p] for p in group], group, keys, values, scalars, near, far, batch, new_tokens, heads_local
        )
        partial += [o if p == 0 else xor_blk(o, p, blocks) for p, o in zip(group, outs)]
    plane = merge(partial, heads_local, head_dim, False)
    pieces = [plane[f * rows_dev : (f + 1) * rows_dev] for f in range(far)]
    pieces = [pieces[0]] + [xor_blk(pieces[f], f * near, blocks) for f in range(1, far)]
    attn = merge(pieces, heads_local, head_dim, True)

    mine = out_projection(gather(attn, near, far, blocks, rows_join), out_weight, scalars, near, far, rows_dev)
    stream, send = stream_step(residual, mine, swap_head(mine), norm_gain[None, :], core[None])

    normed = gather(send, near, far, blocks, stack_join)
    carry = None
    for p in range(near):
        last = p == near - 1
        other = swap_head(normed[p])
        pair = (gate_weight, up_weight)
        if last:
            pair = bring(*pair, spot_late, residual.shape[1], p, near, far)
        carry = feed_chunk(normed[p], other, *pair, spot, carry, p, near, far, width, last, last)
        if p == 0:
            spot_late, carry = lax.optimization_barrier((spot, carry))
    hidden = gather_halves(*carry, near, far, blocks, stack_join)
    carry = None
    for p in range(near):
        carry = down_chunk(hidden[p], down_weight, spot, carry, p, near, far, p == near - 1)
    total = carry.astype(f32) + swap_head(carry).astype(f32)
    return (stream + total).astype(bf16)


def solution(mesh):
    in_specs = (
        P(("groups", "blk"), "head"),
        P("groups", "blk", "head", None),
        P("groups", "blk", "head", None),
        P("groups"),
        P("groups", "blk"),
        P("head", "blk"),
        P("blk"),
        P(None, ("head", "blk")),
        P(None, ("head", "blk")),
        P("head", "blk"),
    )
    out_specs = P("groups", "blk")

    return jax.shard_map(body, mesh=mesh, in_specs=in_specs, out_specs=out_specs, check_vma=False)
```
